512 devices in a mesh: lat: 16 (over y, z_hi), lon: 4 (over x), fold: 8 (over z_lo, core).
Axes of the slice: x: 4, y: 4, z: 16 (z_hi: 4, z_lo: 4; z = z_hi * 4 + z_lo), core: 2. Of those that a mesh axis runs over, the one named last changes fastest.
Arguments:
- field: float32 [8, 12, 640, 2560], P('fold', None, 'lat', 'lon'), may hold values from -6 to 6
- row_shift: int32 [8, 12, 640, 2560], P('fold', None, 'lat', 'lon'), may hold values from -4 to 4
- col_shift: int32 [8, 12, 640, 2560], P('fold', None, 'lat', 'lon'), may hold values from -4 to 4
- row_frac: bfloat16 [8, 12, 640, 2560], P('fold', None, 'lat', 'lon'), may hold values from 0 to 1
- col_frac: bfloat16 [8, 12, 640, 2560], P('fold', None, 'lat', 'lon'), may hold values from 0 to 1
- wave_map: int32 [64], replicated, may hold values from 0 to 1279, as said below
- legendre: float32 [64, 640, 1280], P('lon', 'lat'), may hold values from -0.25 to 0.25
- helm_coef: float32 [48], P('fold'), may hold values from 1e-06 to 0.0001
Outputs:
- spectrum: float32 [48, 4, 16, 2560], P('fold', 'lon', 'lat')
The draws below stay inside these ranges and needn't reach their ends.
Inputs may be any that keep to these rules, and one draw needn't show every extreme that they name: `col_shift`: longitude offset of the departure cell. `wave_map`: distinct zonal wavenumbers.
All inputs are finite; a program needn't handle non-finite values.
Results may differ from the reference program's by a relative error of at most 0.0003.
Values sent between devices are 32-bit elements; how exact they have to be, the bound alone decides.
A program may use at most 64 MiB of HBM per device.

```python
import math
import jax
import jax.numpy as jnp
from jax import lax

LAT_HALF = 640
LON_CELLS = 2560
DEGREES = 1280
SHIFT_MAX = 4
LEVEL_DEV = 12
GROUPS = 8
LEVELS = 48
WAVES_LON = 16
WAVE_SLOTS = 64
N_LON = 4


def draw_wave_map(key, part):
    ordering = jax.random.permutation(key, DEGREES)
    return ordering[:WAVE_SLOTS].astype(jnp.int32)


def plant(result, key, least, largest):
    shape = result.shape
    index_at = [jax.random.randint(jax.random.fold_in(key, axis), (), 0, shape[axis]) for axis in range(len(shape))]
    result = result.at[tuple(index_at)].set(least)
    longest = shape.index(max(shape))
    index_at[longest] = (index_at[longest] + 1) % shape[longest]
    return result.at[tuple(index_at)].set(largest)


def level_of(key, extent, split, smallest, top_value):
    def one(dim, blocks):
        steps = jax.random.uniform(jax.random.fold_in(jax.random.fold_in(key, 6), dim), (blocks,), jnp.float32, smallest / len(split), top_value / len(split))
        return jnp.repeat(jnp.exp(steps), extent[dim] // blocks).reshape((-1,) + (1,) * (len(extent) - dim - 1))

    level = one(*split[0])
    for cut in split[1:]:
        level = level * one(*cut)
    return level


def gaussian(stream_key, dims, scale, bound, pieces=(), held_as=jnp.bfloat16):
    factor_of = level_of(stream_key, dims, pieces, -0.22, 0.18) if pieces else 1.0
    drawn = jax.random.normal(stream_key, dims, jnp.float32) * scale * factor_of
    return jnp.minimum(jnp.maximum(drawn, -bound), bound).astype(held_as)


def setup_inputs(seed: int = 0) -> dict:
    seeds = jax.random.split(jax.random.key(seed), 9)
    return {
        "field": gaussian(seeds[0], (GROUPS, LEVEL_DEV, LAT_HALF, LON_CELLS), 1.0, 6.0, ((0, 8), (2, 16), (3, 4)), jnp.float32),
        "row_shift": plant(jax.random.randint(seeds[1], (GROUPS, LEVEL_DEV, LAT_HALF, LON_CELLS), 0 - SHIFT_MAX, SHIFT_MAX + 1), jax.random.fold_in(seeds[1], 1), 0 - SHIFT_MAX, SHIFT_MAX).astype(jnp.int32),
        "col_shift": plant(jax.random.randint(seeds[2], (GROUPS, LEVEL_DEV, LAT_HALF, LON_CELLS), 0 - SHIFT_MAX, SHIFT_MAX + 1), jax.random.fold_in(seeds[2], 1), 0 - SHIFT_MAX, SHIFT_MAX).astype(jnp.int32),
        "row_frac": jnp.clip(1.0 * jax.random.uniform(seeds[3], (GROUPS, LEVEL_DEV, LAT_HALF, LON_CELLS), jnp.float32) ** level_of(seeds[3], (GROUPS, LEVEL_DEV, LAT_HALF, LON_CELLS), ((0, 8), (2, 16), (3, 4)), -0.2, 0.2), 0.0, 1.0).astype(jnp.bfloat16),
        "col_frac": jnp.clip(1.0 * jax.random.uniform(seeds[4], (GROUPS, LEVEL_DEV, LAT_HALF, LON_CELLS), jnp.float32) ** level_of(seeds[4], (GROUPS, LEVEL_DEV, LAT_HALF, LON_CELLS), ((0, 8), (2, 16), (3, 4)), -0.2, 0.2), 0.0, 1.0).astype(jnp.bfloat16),
        "wave_map": draw_wave_map(jax.random.fold_in(seeds[8], 71), 0),
        "legendre": gaussian(seeds[6], (WAVE_SLOTS, LAT_HALF, DEGREES), LAT_HALF ** -0.5, 0.25, ((0, 4), (1, 16)), jnp.float32),
        "helm_coef": jnp.clip(jnp.exp(math.log(0.0001) - 4.6051702 * jax.random.uniform(seeds[7], (LEVELS,), jnp.float32) ** level_of(seeds[7], (LEVELS,), ((0, 8),), -0.2, 0.2)), 9.999999974752427e-07, 0.0001),
    }


def cubic_weights(fraction):
    return (-fraction * (fraction - 1.0) * (fraction - 2.0) / 6.0, (fraction + 1.0) * (fraction - 1.0) * (fraction - 2.0) / 2.0, -(fraction + 1.0) * fraction * (fraction - 2.0) / 2.0, (fraction + 1.0) * fraction * (fraction - 1.0) / 6.0)

def interpolate(padded, row_shift, col_shift, row_frac, col_frac, margin):
    levels, rows, cols = row_shift.shape
    width = cols + 2 * margin
    flat = padded.reshape(levels, -1)
    row_base = lax.broadcasted_iota(jnp.int32, (levels, rows, cols), 1) + row_shift + (margin - 1)
    col_base = lax.broadcasted_iota(jnp.int32, (levels, rows, cols), 2) + col_shift + (margin - 1)
    start_index = (row_base * width + col_base).reshape(levels, -1).astype(jnp.int32)
    row_weights = cubic_weights(row_frac.astype(jnp.float32).reshape(levels, -1))
    col_weights = cubic_weights(col_frac.astype(jnp.float32).reshape(levels, -1))
    total = jnp.zeros(start_index.shape, jnp.float32)
    for row_step in range(4):
        line = jnp.zeros(start_index.shape, jnp.float32)
        for col_step in range(4):
            taken = jnp.take_along_axis(flat, start_index + (row_step * width + col_step), axis=1)
            line = line + col_weights[col_step] * taken
        total = total + row_weights[row_step] * line
    return total.reshape(levels, rows, cols)

def zonal_table(waves, first_col, count_cols, lon_total):
    col_ids = first_col + lax.iota(jnp.int32, count_cols)
    phase = col_ids[:, None] * waves[None, :] % lon_total
    angle = phase.astype(jnp.float32) * (2.0 * math.pi / lon_total)
    return jnp.stack([jnp.cos(angle), -jnp.sin(angle)], axis=1) / math.sqrt(lon_total)

def reference(field, row_shift, col_shift, row_frac, col_frac, wave_map, legendre, helm_coef):
    margin = SHIFT_MAX + 2
    blocks = GROUPS // 2
    fields = field.reshape(blocks, 2, LEVEL_DEV, LAT_HALF, LON_CELLS)
    opposite = fields[:, ::-1]
    band = opposite[:, :, :, ::-1, :][:, :, :, :margin, :]
    polar = jnp.zeros((blocks, 2, LEVEL_DEV, margin, LON_CELLS), jnp.float32)
    extended = jnp.concatenate([polar, fields, band], axis=3)
    extended = jnp.concatenate([extended[..., -margin:], extended, extended[..., :margin]], axis=4)
    number = blocks * 2 * LEVEL_DEV

    def one_field(items):
        padded, shift_rows, shift_cols, frac_rows, frac_cols = items
        return interpolate(padded[None], shift_rows[None], shift_cols[None], frac_rows[None], frac_cols[None], margin)[0]
    gridded = lax.map(one_field, (extended.reshape(number, LAT_HALF + 2 * margin, LON_CELLS + 2 * margin), row_shift.reshape(number, LAT_HALF, LON_CELLS), col_shift.reshape(number, LAT_HALF, LON_CELLS), row_frac.reshape(number, LAT_HALF, LON_CELLS), col_frac.reshape(number, LAT_HALF, LON_CELLS)))
    gridded = gridded.reshape(blocks, 2, LEVEL_DEV, LAT_HALF, LON_CELLS)
    even = (gridded[:, 0] + gridded[:, 1]).reshape(LEVELS, LAT_HALF, LON_CELLS)
    odd = (gridded[:, 0] - gridded[:, 1]).reshape(LEVELS, LAT_HALF, LON_CELLS)
    table = zonal_table(wave_map, 0, LON_CELLS, LON_CELLS)
    zonal_even = jnp.einsum('lkx,xqs->lsqk', even, table, precision=lax.Precision.HIGHEST)
    zonal_odd = jnp.einsum('lkx,xqs->lsqk', odd, table, precision=lax.Precision.HIGHEST)
    sum_even = jnp.einsum('lsqk,skn->lsqn', zonal_even, legendre, precision=lax.Precision.HIGHEST)
    sum_odd = jnp.einsum('lsqk,skn->lsqn', zonal_odd, legendre, precision=lax.Precision.HIGHEST)
    degrees = jnp.arange(DEGREES, dtype=jnp.int32)
    parity = (wave_map[:, None] + degrees[None, :]) % 2 == 0
    keep = (degrees[None, :] >= wave_map[:, None]).astype(jnp.float32)
    legendre_sum = jnp.where(parity[None, :, None, :], sum_even, sum_odd) * keep[None, :, None, :]
    degree_float = degrees.astype(jnp.float32)
    damping = 1.0 + helm_coef[:, None, None, None] * (degree_float * (degree_float + 1.0))[None, None, None, :]
    spectrum = legendre_sum / damping
    return spectrum.reshape(LEVELS, N_LON, WAVES_LON, 2 * DEGREES)
```

```python
import math

import jax
import jax.numpy as jnp
from jax import lax
from jax.experimental import pallas as pl
from jax.experimental.pallas import tpu as pltpu
from jax.sharding import PartitionSpec as P

MESH = pl.DeviceIdType.MESH
F32 = jnp.float32
SHIFTS = [c for c in range(-5, 7) if c != 0]


def lanes():
    return lax.broadcasted_iota(jnp.int32, (8, 128), 1)


def sublanes():
    return lax.broadcasted_iota(jnp.int32, (8, 128), 0)


def shifted_block(raw, store):
    lane = lanes()
    for t in range(5):
        store(25 + t, raw[t + 1])
    for c in SHIFTS:
        use = range(1, 7) if c > 0 else range(0, 6)
        moved = {t: pltpu.roll(raw[t], (-c) % 128, 1) for t in use}
        for t in range(1, 6):
            if c > 0:
                v = jnp.where(lane < 128 - c, moved[t], moved[t + 1])
            else:
                v = jnp.where(lane < -c, moved[t - 1], moved[t])
            store((c + 5) * 5 + t - 1, v)


def cubic(t):
    tm, tp, t2 = t - 1.0, t + 1.0, t - 2.0
    p, r = t * tm, tp * t2
    return (p * t2 * (-1.0 / 6.0), r * tm * 0.5, r * t * (-0.5), p * tp * (1.0 / 6.0))


def interp_tile(load, rb, rs, cs, u, v):
    idx = sublanes() + rs + 4
    low = idx < 8
    idx = idx & 7
    wr = cubic(u)
    s = cs + 4
    b0, b1, b2, b3 = (s & 1) != 0, (s & 2) != 0, (s & 4) != 0, s >= 8
    take = lambda x: jnp.take_along_axis(x, idx, axis=0, mode="promise_in_bounds")
    line, xs, ys = [], [], []
    for j in range(12):
        acc = None
        for a in range(4):
            g = jnp.where(low, take(load(j, rb * 8 + 3 + a)), take(load(j, rb * 8 + 11 + a))) * wr[a]
            acc = g if acc is None else acc + g
        line.append(acc)
        if 1 <= j <= 10:
            xs.append(jnp.where(b0, line[j], line[j - 1]))
            q = len(xs) - 1
            if q >= 2:
                ys.append(jnp.where(b1, xs[q], xs[q - 2]))
    wc = cubic(v)
    out = None
    for b in range(4):
        z = jnp.where(b2, ys[b + 4], ys[b])
        z = jnp.where(b3, line[b + 8], z)
        out = wc[b] * z if out is None else out + wc[b] * z
    return out


def three_pass(lh, ll, rh, rl, dims):
    dot = lambda a, b: lax.dot_general(a, b, dims, preferred_element_type=F32)
    return dot(lh, rh) + (dot(lh, rl) + dot(ll, rh))


def split(x):
    hi = x.astype(jnp.bfloat16)
    return hi, (x - hi.astype(F32)).astype(jnp.bfloat16)


def grid_kernel(
    n_lat, n_lon,
    field, rsh, csh, rfr, cfr, tab, out,
    raw, rs_v, cs_v, rf_v, cf_v, tops, bots, mirs, cpack, top, bot, ccorn, moved, grid,
    loc_sem, in_sem, cs_sem, cr_sem, ts_sem, tr_sem, bs_sem, br_sem, ks_sem, kr_sem,
):
    lat, lon, fold = lax.axis_index("lat"), lax.axis_index("lon"), lax.axis_index("fold")
    up, down = lax.rem(lat + n_lat - 1, n_lat), lax.rem(lat + 1, n_lat)
    left, right = lax.rem(lon + n_lon - 1, n_lon), lax.rem(lon + 1, n_lon)
    mate = fold + 1 - 2 * lax.rem(fold, 2)
    first, last = lat == 0, lat == n_lat - 1
    levels = raw.shape[0]
    chunks = levels // 4

    fetch = [
        pltpu.make_async_copy(field.at[pl.ds(4 * c, 4)], raw.at[pl.ds(4 * c, 4), :, pl.ds(128, 640)], loc_sem.at[c])
        for c in range(chunks)
    ]
    for c in fetch:
        c.start()
    loads = [pltpu.make_async_copy(a, b, in_sem.at[i]) for i, (a, b) in enumerate(((rsh, rs_v), (csh, cs_v), (rfr, rf_v), (cfr, cf_v)))]
    for c in loads:
        c.start()

    barrier = pltpu.get_barrier_semaphore()
    peers = [{"lat": a, "lon": b, "fold": fold} for a in (up, down) for b in (left, lon, right)]
    peers += [{"lat": lat, "lon": b, "fold": mate} for b in (left, lon, right)]
    peers += [{"lat": lat, "lon": b, "fold": fold} for b in (left, right)]
    for p in peers:
        pl.semaphore_signal(barrier, inc=1, device_id=p, device_id_type=MESH)

    def pack_rows(c):
        for l in range(4 * c, 4 * c + 4):
            for t in range(5):
                tile = pl.ds(128 + 128 * t, 128)
                tops[t, pl.ds(6 * l, 6), :] = raw[l, pl.ds(34, 6), tile]
                bots[t, pl.ds(6 * l, 6), :] = raw[l, pl.ds(0, 6), tile]

        @pl.when(last)
        def _():
            for l in range(4 * c, 4 * c + 4):
                for t in range(5):
                    for r in range(6):
                        mirs[t, pl.ds(6 * l + r, 1), :] = raw[l, pl.ds(39 - r, 1), pl.ds(128 + 128 * t, 128)]

    vregs = levels * 6 // 8

    def pack_corner(k, rows):
        lane = lanes()
        a = b = jnp.zeros((8, 128), F32)
        for i in range(vregs):
            here = (lane >= 12 * i) & (lane < 12 * i + 12)
            a = jnp.where(here, pltpu.roll(rows[0, pl.ds(8 * i, 8), :], 12 * i, 1), a)
            b = jnp.where(here, pltpu.roll(rows[4, pl.ds(8 * i, 8), :], (12 * i + 5) % 128, 1), b)
        cpack[2 * k], cpack[2 * k + 1] = a, b

    def remote(src, dst, ssem, rsem, dev):
        return pltpu.make_async_remote_copy(src_ref=src, dst_ref=dst, send_sem=ssem, recv_sem=rsem, device_id=dev, device_id_type=MESH)

    def cols(c):
        lv = pl.ds(4 * c, 4)
        return (
            remote(raw.at[lv, :, pl.ds(128, 128)], raw.at[lv, :, pl.ds(768, 128)], cs_sem.at[0, c], cr_sem.at[0, c], {"lon": left}),
            remote(raw.at[lv, :, pl.ds(640, 128)], raw.at[lv, :, pl.ds(0, 128)], cs_sem.at[1, c], cr_sem.at[1, c], {"lon": right}),
        )

    def rows(kind, c):
        sl = pl.ds(24 * c, 24)
        if kind == 0:
            return remote(tops.at[:, sl, :], top.at[pl.ds(1, 5), pl.ds(8 + 32 * c, 24), :], ts_sem.at[c], tr_sem.at[c], {"lat": down})
        src, dev = (bots, {"lat": up}) if kind == 1 else (mirs, {"fold": mate})
        return remote(src.at[:, sl, :], bot.at[pl.ds(1, 5), pl.ds(32 * c, 24), :], bs_sem.at[kind - 1, c], br_sem.at[c], dev)

    def corner(kind, side):
        dev = {"lon": right if side else left}
        dev.update(({"lat": down}, {"lat": up}, {"fold": mate})[kind])
        slot = 0 if kind == 0 else 1
        return remote(cpack.at[2 * kind + side], ccorn.at[2 * slot + side], ks_sem.at[2 * kind + side], kr_sem.at[2 * slot + side], dev)

    def each(kind, act):
        cond = (jnp.logical_not(last), jnp.logical_not(first), last)[kind]

        @pl.when(cond)
        def _():
            act()

    for c in range(chunks):
        fetch[c].wait()
        pack_rows(c)
        if c == 0:
            pl.semaphore_wait(barrier, len(peers))
        for kind in range(3):
            each(kind, lambda: rows(kind, c).start())
        for cp in cols(c):
            cp.start()
    for kind, buf in enumerate((tops, bots)):
        pack_corner(kind, buf)
    each(2, lambda: pack_corner(2, mirs))
    for kind in range(3):
        each(kind, lambda: [corner(kind, s).start() for s in range(2)])
    for c in loads:
        c.wait()

    def rows_in(l, blk):
        return [raw[l, pl.ds(8 * (blk - 1), 8), pl.ds(128 * t, 128)] for t in range(7)]

    def build(l, blk, tiles):
        def store(i, v):
            moved[l, i, pl.ds(8 * blk, 8), :] = v
        shifted_block(tiles, store)

    def interp(l, rb):
        row = pl.multiple_of(rb * 8, 8)
        gi, li = lax.div(l, 3), lax.rem(l, 3)
        for t in range(5):
            sl = pl.ds(128 * t, 128)
            args = [r[l, pl.ds(row, 8), sl] for r in (rs_v, cs_v, rf_v, cf_v)]
            val = interp_tile(
                lambda j, r0: moved[l, j * 5 + t, pl.ds(r0, 8), :],
                rb, args[0], args[1], args[2].astype(F32), args[3].astype(F32),
            )
            grid[gi, pl.ds(pl.multiple_of(li * 40 + rb * 8, 8), 8), sl] = val

    for gi in range(levels // 3):
        grid[gi, pl.ds(120, 8), :] = jnp.zeros((8, 640), F32)

    for c in range(chunks):
        for cp in cols(c):
            cp.wait_recv()

        def inner(l, _):
            for blk in range(1, 6):
                build(l, blk, rows_in(l, blk))
            lax.fori_loop(1, 4, lambda rb, x: (interp(l, rb), x)[1], 0)
            return 0

        lax.fori_loop(4 * c, 4 * c + 4, inner, 0)

    @pl.when(first)
    def _():
        top[...] = jnp.zeros_like(top)

    each_in = lambda act: pl.when(jnp.logical_not(first))(act)
    for c in range(chunks):
        each_in(lambda: rows(0, c).wait_recv())
        rows(1, c).wait_recv()
        if c == 0:
            each_in(lambda: [corner(0, s).wait_recv() for s in range(2)] and None)
            for s in range(2):
                corner(1, s).wait_recv()
            for slot, buf, off in ((0, top, 8), (1, bot, 0)):
                def unpack(slot=slot, buf=buf, off=off):
                    to_right, to_left = ccorn[2 * slot], ccorn[2 * slot + 1]
                    for i in range(vregs):
                        sl = pl.ds(off + 8 * i + 8 * (i // 3), 8)
                        buf[6, sl, :] = pltpu.roll(to_right, (-12 * i) % 128, 1)
                        buf[0, sl, :] = pltpu.roll(to_left, (123 - 12 * i) % 128, 1)
                if slot == 0:
                    each_in(unpack)
                else:
                    unpack()

        def outer(l, _):
            build(l, 0, [top[t, pl.ds(6 * l + 8 * c + 6, 8), :] for t in range(7)])
            build(l, 6, [bot[t, pl.ds(6 * l + 8 * c, 8), :] for t in range(7)])
            lax.fori_loop(0, 2, lambda i, x: (interp(l, 4 * i), x)[1], 0)
            return 0

        lax.fori_loop(4 * c, 4 * c + 4, outer, 0)

    th, tl = split(tab[...])
    for gi in range(levels // 3):
        gh, gl = split(grid[gi])
        out[:, pl.ds(128 * gi, 128)] = three_pass(th, tl, gh, gl, (((1,), (1,)), ((), ())))

    for c in range(chunks):
        for cp in cols(c):
            cp.wait_send()
        for kind in range(3):
            each(kind, lambda: rows(kind, c).wait_send())
    for kind in range(3):
        each(kind, lambda: [corner(kind, s).wait_send() for s in range(2)] and None)


def grid_stage(field, rsh, csh, rfr, cfr, tab, n_lat, n_lon):
    levels, rows, cols = field.shape
    any_spec = pl.BlockSpec(memory_space=pl.ANY)
    vm = pl.BlockSpec(memory_space=pltpu.VMEM)
    c = levels // 4
    V = pltpu.VMEM
    dma = pltpu.SemaphoreType.DMA
    import functools
    return pl.pallas_call(
        functools.partial(grid_kernel, n_lat, n_lon),
        out_shape=jax.ShapeDtypeStruct((tab.shape[0], 128 * (levels // 3)), F32),
        in_specs=[any_spec] * 5 + [vm],
        out_specs=vm,
        scratch_shapes=[
            V((levels, rows, cols + 256), F32),
            V(rsh.shape, jnp.int32), V(csh.shape, jnp.int32), V(rfr.shape, jnp.bfloat16), V(cfr.shape, jnp.bfloat16),
            V((5, 6 * levels, 128), F32), V((5, 6 * levels, 128), F32), V((5, 6 * levels, 128), F32),
            V((6, 8, 128), F32),
            V((7, 8 * levels + 8, 128), F32), V((7, 8 * levels + 8, 128), F32),
            V((4, 8, 128), F32),
            V((levels, 60, rows + 16, 128), F32),
            V((levels // 3, 128, cols), F32),
            dma((c,)), dma((4,)), dma((2, c)), dma((2, c)), dma((c,)), dma((c,)), dma((2, c)), dma((c,)), dma((6,)), dma((4,)),
        ],
        compiler_params=pltpu.CompilerParams(collective_id=0, has_side_effects=True, vmem_limit_bytes=60000 * 1024),
        name="grid_stage",
    )(field, rsh, csh, rfr, cfr, tab)


def spectral_kernel(
    n_lon, side,
    wave, coeff, leg, out,
    leg_v, got, zs, part, y1, y2, z1, z2, usum,
    leg_sem, xs_sem, xr_sem, y1s, y1r, y2s, y2r, z1s, z1r, z2s, z2r,
):
    lat, lon, fold = lax.axis_index("lat"), lax.axis_index("lon"), lax.axis_index("fold")
    hemi = lax.rem(fold, 2)
    mate = fold + 1 - 2 * hemi
    yy, zz = lax.div(lat, side), lax.rem(lat, side)
    flip = lambda v: v + 1 - 2 * lax.rem(v, 2)
    pick = lambda a, b: jnp.where(hemi == 0, a, b)
    first_of = lambda v: pick(flip(v), side - 1 - v)
    second_of = lambda v: pick(side - 1 - v, flip(v))
    yp, yq, yo = first_of(yy), second_of(yy), lax.rem(yy + 2, side)
    zp, zq, zo = first_of(zz), second_of(zz), lax.rem(zz + 2, side)

    fetch = pltpu.make_async_copy(leg, leg_v, leg_sem)
    fetch.start()

    barrier = pltpu.get_barrier_semaphore()
    group = [(d, e) for d in range(n_lon) for e in range(2) if d or e]
    peers = [{"lon": lax.rem(lon + d, n_lon), "fold": mate if e else fold} for d, e in group]
    peers += [{"lat": yp * side + zz}, {"lat": yq * side + zz}, {"lat": yy * side + zp}, {"lat": yy * side + zq}]
    for p in peers:
        pl.semaphore_signal(barrier, inc=1, device_id=p, device_id_type=MESH)
    pl.semaphore_wait(barrier, len(peers))

    def remote(src, dst, ssem, rsem, dev):
        return pltpu.make_async_remote_copy(src_ref=src, dst_ref=dst, send_sem=ssem, recv_sem=rsem, device_id=dev, device_id_type=MESH)

    def block(d, e):
        other = lax.rem(lon + d, n_lon)
        h = hemi if e == 0 else 1 - hemi
        return coeff.at[pl.ds(pl.multiple_of(other * 32, 32), 32), pl.ds(pl.multiple_of(h * 256, 256), 256)]

    swap = [remote(block(d, e), got.at[2 * d + e], xs_sem.at[2 * d + e], xr_sem.at[2 * d + e], p) for (d, e), p in zip(group, peers)]
    for s in swap:
        s.start()
    same = block(0, 0)[...]
    for s in swap:
        s.wait_recv()
    for d in range(1, n_lon):
        same = same + got[2 * d]
    other = got[1]
    for d in range(1, n_lon):
        other = other + got[2 * d + 1]
    sign = (1 - 2 * hemi).astype(F32)
    pair = (same + other, sign * (same - other))

    zs[...] = jnp.zeros_like(zs)
    for e in range(2):
        for lv in range(6):
            z = pair[e][:, 128 * (lv // 3) : 128 * (lv // 3) + 128]
            if lv % 3:
                z = pltpu.roll(z, 128 - 40 * (lv % 3), 1)
            for q in range(2):
                zs[pl.ds(16 * e + 6 * q + lv, 16, stride=32), :] = z[16 * q : 16 * q + 16]
    fetch.wait()

    odd_lane = lax.broadcasted_iota(jnp.int32, (16, 640), 1)

    def legendre(slot):
        lhs = zs[pl.ds(pl.multiple_of(slot * 32, 32), 32), :]
        m = wave[lon * 16 + slot]
        a_h, a_l = split(lhs[:, :40])
        b_h, b_l = split(pltpu.roll(lhs, 4, 0)[:, :40])
        even = ((odd_lane + m) & 1) == 0
        dims = (((1,), (0,)), ((), ()))
        r_h, r_l = split(leg_v[slot, :, :640])
        a = three_pass(a_h, a_l, r_h, r_l, dims)
        a = jnp.where(even, a[:16], a[16:])
        r_h, r_l = split(leg_v[slot, :, 640:])
        b = three_pass(b_h, b_l, r_h, r_l, dims)
        b = jnp.where(even, b[:16], b[16:])
        part[slot, pl.ds(0, 8), :] = a[:8]
        sub = lax.broadcasted_iota(jnp.int32, (8, 640), 0)
        part[slot, pl.ds(8, 8), :] = jnp.where(sub < 4, a[8:], b[:8])
        part[slot, pl.ds(16, 8), :] = b[8:]

    zorder = (zp, zo, zq, zz)

    def ystep1(k):
        zt = zorder[k]
        return [
            remote(part.at[yt * side + zt], y1.at[k, i], y1s.at[k, i], y1r.at[k, i], {"lat": yp * side + zz})
            for i, yt in enumerate((yp, yo))
        ]

    def ystep2(k):
        return remote(part.at[yq * side + zorder[k]], y2.at[k], y2s.at[k], y2r.at[k], {"lat": yq * side + zz})

    for k in range(4):
        for yt in (yp, yo):
            legendre(yt * side + zorder[k])
        for s in ystep1(k):
            s.start()
    for k in range(4):
        for yt in (yq, yy):
            legendre(yt * side + zorder[k])
    zstep1 = [remote(usum.at[i], z1.at[i], z1s.at[i], z1r.at[i], {"lat": yy * side + zp}) for i in range(2)]
    zstep2 = remote(usum.at[2], z2, z2s, z2r, {"lat": yy * side + zq})

    def after1(k):
        for s in ystep1(k):
            s.wait_recv()
        send = yq * side + zorder[k]
        part[send] = part[send] + y1[k, 1]
        ystep2(k).start()

    def after2(k):
        ystep2(k).wait_recv()
        usum[k] = (part[yy * side + zorder[k]] + y1[k, 0]) + y2[k]

    after1(0)
    after1(1)
    after2(0)
    zstep1[0].start()
    after1(2)
    after2(1)
    zstep1[1].start()
    after1(3)
    after2(2)
    zstep1[1].wait_recv()
    usum[2] = usum[2] + z1[1]
    zstep2.start()
    after2(3)
    zstep1[0].wait_recv()
    total = usum[3] + z1[0]
    zstep2.wait_recv()
    total = total + z2[...]
    for hn in range(2):
        for q in range(2):
            out[:, pl.ds(1280 * q + 640 * hn, 640)] = total[12 * hn + 6 * q : 12 * hn + 6 * q + 6]
    for s in swap:
        s.wait_send()
    for k in range(4):
        for s in ystep1(k):
            s.wait_send()
        ystep2(k).wait_send()
    for s in zstep1:
        s.wait_send()
    zstep2.wait_send()


def spectral_stage(wave, coeff, leg, n_lon, side):
    import functools
    any_spec = pl.BlockSpec(memory_space=pl.ANY)
    V = pltpu.VMEM
    dma = pltpu.SemaphoreType.DMA
    vm = pl.BlockSpec(memory_space=V)
    blk = (24, 640)
    return pl.pallas_call(
        functools.partial(spectral_kernel, n_lon, side),
        out_shape=jax.ShapeDtypeStruct((6, 2560), F32),
        in_specs=[pl.BlockSpec(memory_space=pltpu.SMEM), vm, any_spec],
        out_specs=vm,
        scratch_shapes=[
            V(leg.shape, F32), V((8, 32, 256), F32), V((512, 128), F32), V((16,) + blk, F32),
            V((4, 2) + blk, F32), V((4,) + blk, F32), V((2,) + blk, F32), V(blk, F32), V((4,) + blk, F32),
            dma(()), dma((8,)), dma((8,)), dma((4, 2)), dma((4, 2)), dma((4,)), dma((4,)), dma((2,)), dma((2,)), dma(()), dma(()),
        ],
        compiler_params=pltpu.CompilerParams(collective_id=1, has_side_effects=True, vmem_limit_bytes=32000 * 1024),
        name="spectral_stage",
    )(wave, coeff, leg)


def zonal_table(waves, first_col, cols, lon_total, groups):
    col = first_col + lax.iota(jnp.int32, cols)
    angle = (waves[:, None] * col[None, :] % lon_total).astype(F32) * (2.0 * math.pi / lon_total)
    both = jnp.stack([jnp.cos(angle), -jnp.sin(angle)], axis=0) / math.sqrt(lon_total)
    return both.reshape(2, groups, -1, cols).transpose(1, 0, 2, 3).reshape(-1, cols)


def local(field, row_shift, col_shift, row_frac, col_frac, wave_map, legendre, helm_coef):
    n_lat, n_lon = lax.axis_size("lat"), lax.axis_size("lon")
    cols = field.shape[3]
    tab = zonal_table(wave_map, lax.axis_index("lon") * cols, cols, cols * n_lon, n_lon)
    coeff = grid_stage(field[0], row_shift[0], col_shift[0], row_frac[0], col_frac[0], tab, n_lat, n_lon)
    sums = spectral_stage(wave_map, coeff, legendre, n_lon, math.isqrt(n_lat))
    degree = lax.iota(jnp.int32, 1280)
    m = wave_map[lax.axis_index("lon") * 16 + lax.axis_index("lat")]
    keep = jnp.tile(degree >= m, 2)
    d = jnp.tile(degree.astype(F32), 2)
    damping = 1.0 + helm_coef[:, None] * (d * (d + 1.0))[None, :]
    return (jnp.where(keep[None, :], sums, 0.0) / damping)[:, None, None, :]


def solution(mesh):
    in_specs = (
        P("fold", None, "lat", "lon"),
        P("fold", None, "lat", "lon"),
        P("fold", None, "lat", "lon"),
        P("fold", None, "lat", "lon"),
        P("fold", None, "lat", "lon"),
        P(),
        P("lon", "lat", None),
        P("fold"),
    )
    return jax.shard_map(local, mesh=mesh, in_specs=in_specs, out_specs=P("fold", "lon", "lat", None), check_vma=False)
```

```python
import functools
import math

import jax
import jax.numpy as jnp
from jax import lax
from jax.experimental import pallas as pl
from jax.experimental.pallas import tpu as pltpu
from jax.sharding import PartitionSpec as P

MESH = pl.DeviceIdType.MESH
F32 = jnp.float32
SHIFTS = [c for c in range(-5, 7) if c != 0]


def lanes():
    return lax.broadcasted_iota(jnp.int32, (8, 128), 1)


def sublanes():
    return lax.broadcasted_iota(jnp.int32, (8, 128), 0)


def shifted_block(raw, store):
    lane = lanes()
    for t in range(5):
        store(25 + t, raw[t + 1])
    for c in SHIFTS:
        use = range(1, 7) if c > 0 else range(0, 6)
        moved = {t: pltpu.roll(raw[t], (-c) % 128, 1) for t in use}
        for t in range(1, 6):
            if c > 0:
                v = jnp.where(lane < 128 - c, moved[t], moved[t + 1])
            else:
                v = jnp.where(lane < -c, moved[t - 1], moved[t])
            store((c + 5) * 5 + t - 1, v)


def cubic(t):
    tm, tp, t2 = t - 1.0, t + 1.0, t - 2.0
    p, r = t * tm, tp * t2
    return (p * t2 * (-1.0 / 6.0), r * tm * 0.5, r * t * (-0.5), p * tp * (1.0 / 6.0))


def interp_tile(load, rb, rs, cs, u, v):
    idx = sublanes() + rs + 4
    low = idx < 8
    idx = idx & 7
    wr = cubic(u)
    s = cs + 4
    b0, b1, b2, b3 = (s & 1) != 0, (s & 2) != 0, (s & 4) != 0, s >= 8
    take = lambda x: jnp.take_along_axis(x, idx, axis=0, mode="promise_in_bounds")
    line, xs, ys = [], [], []
    for j in range(12):
        acc = None
        for a in range(4):
            g = jnp.where(low, take(load(j, rb * 8 + 3 + a)), take(load(j, rb * 8 + 11 + a))) * wr[a]
            acc = g if acc is None else acc + g
        line.append(acc)
        if 1 <= j <= 10:
            xs.append(jnp.where(b0, line[j], line[j - 1]))
            q = len(xs) - 1
            if q >= 2:
                ys.append(jnp.where(b1, xs[q], xs[q - 2]))
    wc = cubic(v)
    out = None
    for b in range(4):
        z = jnp.where(b2, ys[b + 4], ys[b])
        z = jnp.where(b3, line[b + 8], z)
        out = wc[b] * z if out is None else out + wc[b] * z
    return out


def three_pass(lh, ll, rh, rl, dims):
    dot = lambda a, b: lax.dot_general(a, b, dims, preferred_element_type=F32)
    return dot(lh, rh) + (dot(lh, rl) + dot(ll, rh))


def split(x):
    hi = x.astype(jnp.bfloat16)
    return hi, (x - hi.astype(F32)).astype(jnp.bfloat16)


def order_of_fetch(chunk):
    return (2 * chunk, 6 + 2 * chunk)


def whole_kernel(
    n_lat, n_lon, side,
    wave, helm, field, rsh, csh, rfr, cfr, leg, tab, out,
    raw, rs_v, cs_v, rf_v, cf_v, tops, bots, mirs, cpack, halo, ccorn, moved_a, moved_b, grid, tab_h, tab_l,
    leg_v, leg_h, leg_l, coeff, got, zs, part, y_in, usum, z_in,
    loc_sem, in_sem, leg_sem, tab_sem, cs_sem, cr_sem, ts_sem, tr_sem, bs_sem, br_sem, ks_sem, kr_sem, xs_sem, xr_sem, ys_sem, yr_sem, zs_sem, zr_sem,
):
    lat, lon, fold = lax.axis_index("lat"), lax.axis_index("lon"), lax.axis_index("fold")
    up, down = lax.rem(lat + n_lat - 1, n_lat), lax.rem(lat + 1, n_lat)
    left, right = lax.rem(lon + n_lon - 1, n_lon), lax.rem(lon + 1, n_lon)
    hemi = lax.rem(fold, 2)
    mate = fold + 1 - 2 * hemi
    first, last = lat == 0, lat == n_lat - 1
    yy, zz = lax.div(lat, side), lax.rem(lat, side)
    y_at = [lax.rem(yy + d, side) for d in range(side)]
    z_at = [lax.rem(zz + d, side) for d in range(side)]
    chunks = 3

    def fetch(c, h):
        return pltpu.make_async_copy(
            field.at[pl.ds(order_of_fetch(c)[h], 2)], raw.at[pl.ds(4 * c + 2 * h, 2), :, pl.ds(128, 640)], loc_sem.at[c, h]
        )

    def load(i, c, h):
        src, dst = ((rsh, rs_v), (csh, cs_v), (rfr, rf_v), (cfr, cf_v))[i]
        return pltpu.make_async_copy(src.at[pl.ds(order_of_fetch(c)[h], 2)], dst.at[pl.ds(4 * c + 2 * h, 2)], in_sem.at[i, c, h])

    for c in range(chunks):
        for h in range(2):
            fetch(c, h).start()
    for c in range(chunks):
        for i in range(4):
            for h in range(2):
                load(i, c, h).start()
    leg_fetch = pltpu.make_async_copy(leg, leg_v, leg_sem)
    leg_fetch.start()
    tab_fetch = pltpu.make_async_copy(tab, grid.at[pl.ds(0, 128), :], tab_sem)
    tab_fetch.start()

    barrier = pltpu.get_barrier_semaphore()
    peers = [{"lat": a, "lon": b} for a in (up, down) for b in (left, lon, right)]
    peers += [{"lon": b, "fold": mate} for b in (left, lon, right)]
    group = [(d, e) for d in range(n_lon) for e in range(2) if d or e]
    swap_to = [{"lon": lax.rem(lon + d, n_lon), "fold": mate if e else fold} for d, e in group]
    y_to = [{"lat": y_at[d] * side + zz} for d in range(1, side)]
    z_to = [{"lat": yy * side + z_at[d]} for d in range(1, side)]
    peers += swap_to + y_to + z_to
    for p in peers:
        pl.semaphore_signal(barrier, inc=1, device_id=p, device_id_type=MESH)

    def remote(src, dst, ssem, rsem, dev):
        return pltpu.make_async_remote_copy(src_ref=src, dst_ref=dst, send_sem=ssem, recv_sem=rsem, device_id=dev, device_id_type=MESH)

    def pack_rows(c):
        for l in range(4 * c, 4 * c + 4):
            for t in range(5):
                tile = pl.ds(128 + 128 * t, 128)
                tops[t, pl.ds(6 * l, 6), :] = raw[l, pl.ds(34, 6), tile]
                bots[t, pl.ds(6 * l, 6), :] = raw[l, pl.ds(0, 6), tile]

        @pl.when(last)
        def _():
            for l in range(4 * c, 4 * c + 4):
                for t in range(5):
                    for r in range(6):
                        mirs[t, pl.ds(6 * l + r, 1), :] = raw[l, pl.ds(39 - r, 1), pl.ds(128 + 128 * t, 128)]

    def pack_corner(k, rows):
        lane = lanes()
        a = b = jnp.zeros((8, 128), F32)
        for i in range(9):
            here = (lane >= 12 * i) & (lane < 12 * i + 12)
            a = jnp.where(here, pltpu.roll(rows[0, pl.ds(8 * i, 8), :], 12 * i, 1), a)
            b = jnp.where(here, pltpu.roll(rows[4, pl.ds(8 * i, 8), :], (12 * i + 5) % 128, 1), b)
        cpack[2 * k], cpack[2 * k + 1] = a, b

    def cols(c):
        lv = pl.ds(4 * c, 4)
        return (
            remote(raw.at[lv, :, pl.ds(128, 128)], raw.at[lv, :, pl.ds(768, 128)], cs_sem.at[0, c], cr_sem.at[0, c], {"lon": left}),
            remote(raw.at[lv, :, pl.ds(640, 128)], raw.at[lv, :, pl.ds(0, 128)], cs_sem.at[1, c], cr_sem.at[1, c], {"lon": right}),
        )

    def rows(kind, c):
        sl = pl.ds(pl.multiple_of(24 * c, 8), 24)
        if kind == 0:
            return remote(tops.at[:, sl, :], halo.at[0, pl.ds(1, 5), pl.ds(pl.multiple_of(8 + 32 * c, 8), 24), :], ts_sem.at[c], tr_sem.at[c], {"lat": down})
        src, dev = (bots, {"lat": up}) if kind == 1 else (mirs, {"fold": mate})
        return remote(src.at[:, sl, :], halo.at[1, pl.ds(1, 5), pl.ds(pl.multiple_of(8 + 32 * c, 8), 24), :], bs_sem.at[kind - 1, c], br_sem.at[c], dev)

    def corner(kind, side_):
        dev = {"lon": right if side_ else left}
        dev.update(({"lat": down}, {"lat": up}, {"fold": mate})[kind])
        slot = 0 if kind == 0 else 1
        return remote(cpack.at[2 * kind + side_], ccorn.at[2 * slot + side_], ks_sem.at[2 * kind + side_], kr_sem.at[2 * slot + side_], dev)

    def each(kind, act):
        cond = (jnp.logical_not(last), jnp.logical_not(first), last)[kind]

        @pl.when(cond)
        def _():
            act()

    for c in range(chunks):
        for h in range(2):
            fetch(c, h).wait()
        pack_rows(c)
        if c == 0:
            pl.semaphore_wait(barrier, len(peers))
        for kind in range(3):
            each(kind, lambda: rows(kind, c).start())
        for cp in cols(c):
            cp.start()
    for kind, buf in enumerate((tops, bots)):
        pack_corner(kind, buf)
    each(2, lambda: pack_corner(2, mirs))
    for kind in range(3):
        each(kind, lambda: [corner(kind, s).start() for s in range(2)] and None)

    tab_fetch.wait()
    hi, lo = split(grid[pl.ds(0, 128), :])
    tab_h[...], tab_l[...] = hi, lo
    for half in range(2):
        grid[pl.ds(128 * half + 80, 48), :] = jnp.zeros((48, 640), F32)
    leg_fetch.wait()

    def split_leg(s, x):
        hi, lo = split(leg_v[s])
        leg_h[s], leg_l[s] = hi, lo
        return x

    lax.fori_loop(0, 16, split_leg, 0)

    @pl.when(first)
    def _():
        halo[0] = jnp.zeros_like(halo[0])

    moved = (moved_a, moved_b)

    def build(par, slot, blk, tiles):
        def store(i, v):
            moved[par][slot, i, pl.ds(pl.multiple_of(8 * blk, 8), 8), :] = v
        shifted_block(tiles, store)

    def own_tiles(l, blk):
        return [raw[l, pl.ds(pl.multiple_of(8 * (blk - 1), 8), 8), pl.ds(128 * t, 128)] for t in range(7)]

    def edge_tiles(c, l, e):
        return [halo[e, t, pl.ds(6 * l + 8 * c + 6 + 2 * e, 8), :] for t in range(7)]

    def interp(c, par, i, rb):
        l, slot = 4 * c + 2 * i + par, 2 * c + i
        for t in range(5):
            sl = pl.ds(128 * t, 128)
            args = [r[l, pl.ds(pl.multiple_of(8 * rb, 8), 8), sl] for r in (rs_v, cs_v, rf_v, cf_v)]
            val = interp_tile(
                lambda j, r0: moved[par][slot, j * 5 + t, pl.ds(r0, 8), :],
                rb, args[0], args[1], args[2].astype(F32), args[3].astype(F32),
            )
            grid[pl.ds(pl.multiple_of(128 * i + 40 * par + 8 * rb, 8), 8), sl] = val

    def build_own(c, par, i, blk):
        build(par, 2 * c + i, blk, own_tiles(4 * c + 2 * i + par, blk))

    def build_edge(c, par, i, e):
        build(par, 2 * c + i, 6 * e, edge_tiles(c, 4 * c + 2 * i + par, e))

    def inside(c):
        lax.fori_loop(1, 6, lambda blk, x: (build_own(c, 0, 0, blk), x)[1], 0)

        def pair(i, x):
            for par in range(2):
                nxt = 1 if par else i

                def step(rb, y):
                    build_own(c, 1 - par, nxt, rb)
                    build_own(c, 1 - par, nxt, rb + 2)
                    interp(c, par, i, rb)
                    return y

                lax.fori_loop(1, 4, step, 0)
            return x

        lax.fori_loop(0, 2, pair, 0)

    def edges(c):
        lax.fori_loop(0, 2, lambda e, x: (build_edge(c, 0, 0, e), x)[1], 0)

        def pair(i, x):
            for par in range(2):
                nxt = 1 if par else i

                def step(e, y):
                    build_edge(c, 1 - par, nxt, e)
                    interp(c, par, i, 4 * e)
                    return y

                lax.fori_loop(0, 2, step, 0)
            return x

        lax.fori_loop(0, 2, pair, 0)

    def unpack_corners(slot):
        to_right, to_left = ccorn[2 * slot], ccorn[2 * slot + 1]
        for i in range(9):
            sl = pl.ds(8 + 8 * i + 8 * (i // 3), 8)
            halo[slot, 6, sl, :] = pltpu.roll(to_right, (-12 * i) % 128, 1)
            halo[slot, 0, sl, :] = pltpu.roll(to_left, (123 - 12 * i) % 128, 1)

    not_first = lambda act: pl.when(jnp.logical_not(first))(act)

    def swap(c, d, e, dev):
        other = lax.rem(lon + d, n_lon)
        h = hemi if e == 0 else 1 - hemi
        src = coeff.at[c, pl.ds(pl.multiple_of(other * 32, 32), 32), pl.ds(pl.multiple_of(h * 128, 128), 128)]
        return remote(src, got.at[c, 2 * d + e], xs_sem.at[c, 2 * d + e], xr_sem.at[c, 2 * d + e], dev)

    swaps = lambda c: [swap(c, d, e, dev) for (d, e), dev in zip(group, swap_to)]

    def grid_part(c):
        for cp in cols(c):
            cp.wait_recv()
        for i in range(4):
            for h in range(2):
                load(i, c, h).wait()
        inside(c)
        not_first(lambda: rows(0, c).wait_recv())
        rows(1, c).wait_recv()

        @pl.when(c == 0)
        def _():
            for s in range(2):
                not_first(lambda: corner(0, s).wait_recv())
                corner(1, s).wait_recv()
            not_first(lambda: unpack_corners(0))
            unpack_corners(1)

        edges(c)
        gh, gl = split(grid[...])
        coeff[c] = three_pass(tab_h[...], tab_l[...], gh, gl, (((1,), (1,)), ((), ())))
        for s in swaps(c):
            s.start()

    def y_copy(c, d):
        return remote(part.at[c, pl.ds(4 * d, 4)], y_in.at[c, d - 1], ys_sem.at[c, d - 1], yr_sem.at[c, d - 1], y_to[d - 1])

    def z_copy(c, d):
        return remote(usum.at[c, d], z_in.at[c, d - 1], zs_sem.at[c, d - 1], zr_sem.at[c, d - 1], z_to[d - 1])

    others = range(1, side)
    y_send = lambda c: [y_copy(c, d) for d in others]
    z_send = lambda c: [z_copy(c, d) for d in others]
    sub_w = lax.broadcasted_iota(jnp.int32, (8, 640), 0)
    lane_w = lax.broadcasted_iota(jnp.int32, (8, 640), 1)

    def legendre_part(c):
        for s in swaps(c):
            s.wait_recv()
        same = coeff[c, pl.ds(pl.multiple_of(lon * 32, 32), 32), pl.ds(pl.multiple_of(hemi * 128, 128), 128)]
        other = got[c, 1]
        for d in range(1, n_lon):
            same = same + got[c, 2 * d]
            other = other + got[c, 2 * d + 1]
        sign = (1 - 2 * hemi).astype(F32)
        for e, z in enumerate((same + other, sign * (same - other))):
            for lv in range(2):
                moved_z = pltpu.roll(z, 88, 1) if lv else z
                for q in range(2):
                    for dup in range(2):
                        zs[pl.ds(8 * e + 4 * dup + 2 * q + lv, 16, stride=16), :] = moved_z[16 * q : 16 * q + 16]

        dims = (((1,), (0,)), ((), ()))

        def one(k, x):
            slot = lax.rem(yy + lax.div(k, side), side) * side + lax.rem(zz + lax.rem(k, side), side)
            m = wave[lon * 16 + slot]
            l_h, l_l = split(zs[pl.ds(pl.multiple_of(slot * 16, 16), 16), :][:, :40])
            even = ((lane_w + m) & 1) == 0
            res = []
            for hn in range(2):
                sl = pl.ds(640 * hn, 640)
                v = three_pass(l_h, l_l, leg_h[slot, :, sl], leg_l[slot, :, sl], dims)
                res.append(jnp.where(even, v[:8], v[8:]))
            part[c, k] = jnp.where(sub_w < 4, res[0], res[1])
            return x

        for d in (2, 1, 3, 0):
            lax.fori_loop(4 * d, 4 * d + 4, one, 0)
            if d:
                y_copy(c, d).start()

    def y_part(c):
        for s in y_send(c):
            s.wait_recv()
        for d in (2, 1, 3, 0):
            usum[c, d] = (part[c, d] + y_in[c, 0, d]) + (y_in[c, 1, d] + y_in[c, 2, d])
            if d:
                z_copy(c, d).start()

    def z_part(c):
        for s in z_send(c):
            s.wait_recv()
        total = (usum[c, 0] + z_in[c, 0]) + (z_in[c, 1] + z_in[c, 2])
        m = wave[lon * 16 + lat]
        degree = lane_w + jnp.where(sub_w < 4, 0, 640)
        h = jnp.where((sub_w & 1) == 0, helm[2 * c], helm[2 * c + 1])
        d = degree.astype(F32)
        total = jnp.where(degree >= m, total, 0.0) / (1.0 + h * (d * (d + 1.0)))
        for hn in range(2):
            for q in range(2):
                out[pl.ds(2 * c, 2), pl.ds(1280 * q + 640 * hn, 640)] = total[4 * hn + 2 * q : 4 * hn + 2 * q + 2]

    def flow(c, x):
        grid_part(c)

        @pl.when(c > 0)
        def _():
            legendre_part(c - 1)

        return x

    lax.fori_loop(0, chunks, flow, 0)
    y_part(0)
    legendre_part(chunks - 1)
    y_part(1)
    z_part(0)
    y_part(2)
    z_part(1)
    z_part(2)

    for c in range(chunks):
        for cp in cols(c):
            cp.wait_send()
        for kind in range(3):
            each(kind, lambda: rows(kind, c).wait_send())
        for s in swaps(c) + y_send(c) + z_send(c):
            s.wait_send()
    for kind in range(3):
        each(kind, lambda: [corner(kind, s).wait_send() for s in range(2)] and None)


def whole(wave, helm, field, rsh, csh, rfr, cfr, leg, tab, n_lat, n_lon):
    levels, rows, cols = field.shape
    V, S = pltpu.VMEM, pltpu.SMEM
    any_spec = pl.BlockSpec(memory_space=pl.ANY)
    sm = pl.BlockSpec(memory_space=S)
    B16, I32 = jnp.bfloat16, jnp.int32
    dma = pltpu.SemaphoreType.DMA
    c = 3
    edge = (5, 6 * levels, 128)
    blk = (8, 640)
    return pl.pallas_call(
        functools.partial(whole_kernel, n_lat, n_lon, math.isqrt(n_lat)),
        out_shape=jax.ShapeDtypeStruct((6, 2560), F32),
        in_specs=[sm, sm] + [any_spec] * 7,
        out_specs=pl.BlockSpec(memory_space=V),
        scratch_shapes=[
            V((levels, rows, cols + 256), F32), V(rsh.shape, I32), V(csh.shape, I32), V(rfr.shape, B16), V(cfr.shape, B16),
            V(edge, F32), V(edge, F32), V(edge, F32), V((6, 8, 128), F32),
            V((2, 7, 8 * levels + 16, 128), F32), V((4, 8, 128), F32),
            V((6, 60, rows + 16, 128), F32), V((6, 60, rows + 16, 128), F32),
            V((256, cols), F32), V((128, cols), B16), V((128, cols), B16),
            V(leg.shape, F32), V(leg.shape, B16), V(leg.shape, B16),
            V((c, 128, 256), F32), V((c, 8, 32, 128), F32), V((256, 128), F32),
            V((c, 16) + blk, F32), V((c, 3, 4) + blk, F32), V((c, 4) + blk, F32), V((c, 3) + blk, F32),
            dma((c, 2)), dma((4, c, 2)), dma(()), dma(()), dma((2, c)), dma((2, c)), dma((c,)), dma((c,)), dma((2, c)), dma((c,)), dma((6,)), dma((4,)),
            dma((c, 8)), dma((c, 8)), dma((c, 3)), dma((c, 3)), dma((c, 3)), dma((c, 3)),
        ],
        compiler_params=pltpu.CompilerParams(collective_id=0, has_side_effects=True, vmem_limit_bytes=60000 * 1024),
        name="whole",
    )(wave, helm, field, rsh, csh, rfr, cfr, leg, tab)


def zonal_table(waves, first_col, cols, lon_total, groups):
    col = first_col + lax.iota(jnp.int32, cols)
    angle = (waves[:, None] * col[None, :] % lon_total).astype(F32) * (2.0 * math.pi / lon_total)
    both = jnp.stack([jnp.cos(angle), -jnp.sin(angle)], axis=0) / math.sqrt(lon_total)
    return both.reshape(2, groups, -1, cols).transpose(1, 0, 2, 3).reshape(-1, cols)


def local(field, row_shift, col_shift, row_frac, col_frac, wave_map, legendre, helm_coef):
    n_lat, n_lon = lax.axis_size("lat"), lax.axis_size("lon")
    cols = field.shape[3]
    tab = zonal_table(wave_map, lax.axis_index("lon") * cols, cols, cols * n_lon, n_lon)
    result = whole(wave_map, helm_coef, field[0], row_shift[0], col_shift[0], row_frac[0], col_frac[0], legendre, tab, n_lat, n_lon)
    return result[:, None, None, :]


def solution(mesh):
    in_specs = (
        P("fold", None, "lat", "lon"),
        P("fold", None, "lat", "lon"),
        P("fold", None, "lat", "lon"),
        P("fold", None, "lat", "lon"),
        P("fold", None, "lat", "lon"),
        P(),
        P("lon", "lat", None),
        P("fold"),
    )
    return jax.shard_map(local, mesh=mesh, in_specs=in_specs, out_specs=P("fold", "lon", "lat", None), check_vma=False)
```

```python
import functools
import math

import jax
import jax.numpy as jnp
from jax import lax
from jax.experimental import pallas as pl
from jax.experimental.pallas import tpu as pltpu
from jax.sharding import PartitionSpec as P

MESH = pl.DeviceIdType.MESH
F32 = jnp.float32
SHIFTS = [c for c in range(-5, 7) if c != 0]


def lanes():
    return lax.broadcasted_iota(jnp.int32, (8, 128), 1)


def sublanes():
    return lax.broadcasted_iota(jnp.int32, (8, 128), 0)


def shifted_block(raw, store):
    lane = lanes()
    for t in range(5):
        store(25 + t, raw[t + 1])
    for c in SHIFTS:
        use = range(1, 7) if c > 0 else range(0, 6)
        moved = {t: pltpu.roll(raw[t], (-c) % 128, 1) for t in use}
        for t in range(1, 6):
            if c > 0:
                v = jnp.where(lane < 128 - c, moved[t], moved[t + 1])
            else:
                v = jnp.where(lane < -c, moved[t - 1], moved[t])
            store((c + 5) * 5 + t - 1, v)


def cubic(t):
    tm, tp, t2 = t - 1.0, t + 1.0, t - 2.0
    p, r = t * tm, tp * t2
    return (p * t2 * (-1.0 / 6.0), r * tm * 0.5, r * t * (-0.5), p * tp * (1.0 / 6.0))


def interp_tile(load, rb, rs, cs, u, v):
    idx = sublanes() + rs + 4
    low = idx < 8
    idx = idx & 7
    wr = cubic(u)
    s = cs + 4
    b0, b1, b2, b3 = (s & 1) != 0, (s & 2) != 0, (s & 4) != 0, s >= 8
    take = lambda x: jnp.take_along_axis(x, idx, axis=0, mode="promise_in_bounds")
    line, xs, ys = [], [], []
    for j in range(12):
        acc = None
        for a in range(4):
            g = jnp.where(low, take(load(j, rb * 8 + 3 + a)), take(load(j, rb * 8 + 11 + a))) * wr[a]
            acc = g if acc is None else acc + g
        line.append(acc)
        if 1 <= j <= 10:
            xs.append(jnp.where(b0, line[j], line[j - 1]))
            q = len(xs) - 1
            if q >= 2:
                ys.append(jnp.where(b1, xs[q], xs[q - 2]))
    wc = cubic(v)
    out = None
    for b in range(4):
        z = jnp.where(b2, ys[b + 4], ys[b])
        z = jnp.where(b3, line[b + 8], z)
        out = wc[b] * z if out is None else out + wc[b] * z
    return out


def three_pass(lh, ll, rh, rl, dims):
    dot = lambda a, b: lax.dot_general(a, b, dims, preferred_element_type=F32)
    n = lh.shape[0]
    both = dot(jnp.concatenate([lh, ll], axis=0), rh)
    return both[:n] + (dot(lh, rl) + both[n:])


def split(x):
    hi = x.astype(jnp.bfloat16)
    return hi, (x - hi.astype(F32)).astype(jnp.bfloat16)


def order_of_fetch(chunk):
    return (2 * chunk, 6 + 2 * chunk)


def whole_kernel(
    n_lat, n_lon, side,
    wave, helm, field, rsh, csh, rfr, cfr, leg, out,
    raw, rs_v, cs_v, rf_v, cf_v, tops, bots, mirs, cpack, halo, ccorn, moved_a, moved_b, grid, tab_h, tab_l,
    leg_v, leg_h, leg_l, coeff, got, zs, part, y_in, usum, z_in,
    loc_sem, in_sem, leg_sem, cs_sem, cr_sem, ts_sem, tr_sem, bs_sem, br_sem, ks_sem, kr_sem, xs_sem, xr_sem, ys_sem, yr_sem, zs_sem, zr_sem,
):
    lat, lon, fold = lax.axis_index("lat"), lax.axis_index("lon"), lax.axis_index("fold")
    up, down = lax.rem(lat + n_lat - 1, n_lat), lax.rem(lat + 1, n_lat)
    left, right = lax.rem(lon + n_lon - 1, n_lon), lax.rem(lon + 1, n_lon)
    hemi = lax.rem(fold, 2)
    mate = fold + 1 - 2 * hemi
    first, last = lat == 0, lat == n_lat - 1
    yy, zz = lax.div(lat, side), lax.rem(lat, side)
    y_at = [lax.rem(yy + d, side) for d in range(side)]
    z_at = [lax.rem(zz + d, side) for d in range(side)]
    chunks = 3

    def fetch(c, h):
        return pltpu.make_async_copy(
            field.at[pl.ds(order_of_fetch(c)[h], 2)], raw.at[pl.ds(4 * c + 2 * h, 2), :, pl.ds(128, 640)], loc_sem.at[c, h]
        )

    def load(i, c, h):
        src, dst = ((rsh, rs_v), (csh, cs_v), (rfr, rf_v), (cfr, cf_v))[i]
        return pltpu.make_async_copy(src.at[pl.ds(order_of_fetch(c)[h], 2)], dst.at[pl.ds(4 * c + 2 * h, 2)], in_sem.at[i, c, h])

    for c in range(chunks):
        for h in range(2):
            fetch(c, h).start()
    for c in range(chunks):
        for i in range(4):
            for h in range(2):
                load(i, c, h).start()
    leg_fetch = pltpu.make_async_copy(leg, leg_v, leg_sem)
    leg_fetch.start()
    barrier = pltpu.get_barrier_semaphore()
    peers = [{"lat": a, "lon": b} for a in (up, down) for b in (left, lon, right)]
    peers += [{"lon": b, "fold": mate} for b in (left, lon, right)]
    group = [(d, e) for d in range(n_lon) for e in range(2) if d or e]
    swap_to = [{"lon": lax.rem(lon + d, n_lon), "fold": mate if e else fold} for d, e in group]
    y_to = [{"lat": y_at[d] * side + zz} for d in range(1, side)]
    z_to = [{"lat": yy * side + z_at[d]} for d in range(1, side)]
    peers += swap_to + y_to + z_to
    for p in peers:
        pl.semaphore_signal(barrier, inc=1, device_id=p, device_id_type=MESH)

    def remote(src, dst, ssem, rsem, dev):
        return pltpu.make_async_remote_copy(src_ref=src, dst_ref=dst, send_sem=ssem, recv_sem=rsem, device_id=dev, device_id_type=MESH)

    def pack_rows(c):
        for l in range(4 * c, 4 * c + 4):
            for t in range(5):
                tile = pl.ds(128 + 128 * t, 128)
                tops[t, pl.ds(6 * l, 6), :] = raw[l, pl.ds(34, 6), tile]
                bots[t, pl.ds(6 * l, 6), :] = raw[l, pl.ds(0, 6), tile]

        @pl.when(last)
        def _():
            for l in range(4 * c, 4 * c + 4):
                for t in range(5):
                    for r in range(6):
                        mirs[t, pl.ds(6 * l + r, 1), :] = raw[l, pl.ds(39 - r, 1), pl.ds(128 + 128 * t, 128)]

    def pack_corner(k, rows):
        lane = lanes()
        a = b = jnp.zeros((8, 128), F32)
        for i in range(9):
            here = (lane >= 12 * i) & (lane < 12 * i + 12)
            a = jnp.where(here, pltpu.roll(rows[0, pl.ds(8 * i, 8), :], 12 * i, 1), a)
            b = jnp.where(here, pltpu.roll(rows[4, pl.ds(8 * i, 8), :], (12 * i + 5) % 128, 1), b)
        cpack[2 * k], cpack[2 * k + 1] = a, b

    def cols(c):
        lv = pl.ds(4 * c, 4)
        return (
            remote(raw.at[lv, :, pl.ds(128, 128)], raw.at[lv, :, pl.ds(768, 128)], cs_sem.at[0, c], cr_sem.at[0, c], {"lon": left}),
            remote(raw.at[lv, :, pl.ds(640, 128)], raw.at[lv, :, pl.ds(0, 128)], cs_sem.at[1, c], cr_sem.at[1, c], {"lon": right}),
        )

    def rows(kind, c):
        sl = pl.ds(pl.multiple_of(24 * c, 8), 24)
        if kind == 0:
            return remote(tops.at[:, sl, :], halo.at[0, pl.ds(1, 5), pl.ds(pl.multiple_of(8 + 32 * c, 8), 24), :], ts_sem.at[c], tr_sem.at[c], {"lat": down})
        src, dev = (bots, {"lat": up}) if kind == 1 else (mirs, {"fold": mate})
        return remote(src.at[:, sl, :], halo.at[1, pl.ds(1, 5), pl.ds(pl.multiple_of(8 + 32 * c, 8), 24), :], bs_sem.at[kind - 1, c], br_sem.at[c], dev)

    def corner(kind, side_):
        dev = {"lon": right if side_ else left}
        dev.update(({"lat": down}, {"lat": up}, {"fold": mate})[kind])
        slot = 0 if kind == 0 else 1
        return remote(cpack.at[2 * kind + side_], ccorn.at[2 * slot + side_], ks_sem.at[2 * kind + side_], kr_sem.at[2 * slot + side_], dev)

    def each(kind, act):
        cond = (jnp.logical_not(last), jnp.logical_not(first), last)[kind]

        @pl.when(cond)
        def _():
            act()

    sub, lane = sublanes(), lanes()
    for g in range(n_lon):
        for b in range(2):
            m = jnp.zeros((8, 128), jnp.int32)
            for k in range(8):
                m = jnp.where(sub == k, wave[16 * g + 8 * b + k], m)
            for t in range(5):
                turn = (m * (lane + (lon * 640 + 128 * t))).astype(F32)
                turn = turn - jnp.floor(turn * (1.0 / 2560.0)) * 2560.0
                angle = turn * (2.0 * math.pi / 2560.0)
                scale = 1.0 / math.sqrt(2560.0)
                for q, v in enumerate((jnp.cos(angle) * scale, jnp.sin(angle) * -scale)):
                    grid[0, pl.ds(32 * g + 16 * q + 8 * b, 8), pl.ds(128 * t, 128)] = v
    for c in range(chunks):
        for h in range(2):
            fetch(c, h).wait()
        pack_rows(c)
        if c == 0:
            pl.semaphore_wait(barrier, len(peers))
        if c == 0:
            for kind in range(3):
                each(kind, lambda: rows(kind, c).start())
        for cp in cols(c):
            cp.start()
    for kind, buf in enumerate((tops, bots)):
        pack_corner(kind, buf)
    each(2, lambda: pack_corner(2, mirs))
    for kind in range(3):
        each(kind, lambda: [corner(kind, s).start() for s in range(2)] and None)

    hi, lo = split(grid[0, pl.ds(0, 128), :])
    tab_h[...], tab_l[...] = hi, lo
    for c in range(chunks):
        for half in range(2):
            grid[c, pl.ds(128 * half + 80, 48), :] = jnp.zeros((48, 640), F32)
    @pl.when(first)
    def _():
        halo[0] = jnp.zeros_like(halo[0])

    moved = (moved_a, moved_b)

    def build(par, slot, blk, tiles):
        def store(i, v):
            moved[par][slot, i, pl.ds(pl.multiple_of(8 * blk, 8), 8), :] = v
        shifted_block(tiles, store)

    def own_tiles(l, blk):
        return [raw[l, pl.ds(pl.multiple_of(8 * (blk - 1), 8), 8), pl.ds(128 * t, 128)] for t in range(7)]

    def edge_tiles(c, l, e):
        return [halo[e, t, pl.ds(6 * l + 8 * c + 6 + 2 * e, 8), :] for t in range(7)]

    def interp(c, par, i, rb):
        l, slot = 4 * c + 2 * i + par, 2 * c + i
        for t in range(5):
            sl = pl.ds(128 * t, 128)
            args = [r[l, pl.ds(pl.multiple_of(8 * rb, 8), 8), sl] for r in (rs_v, cs_v, rf_v, cf_v)]
            val = interp_tile(
                lambda j, r0: moved[par][slot, j * 5 + t, pl.ds(r0, 8), :],
                rb, args[0], args[1], args[2].astype(F32), args[3].astype(F32),
            )
            grid[c, pl.ds(pl.multiple_of(128 * i + 40 * par + 8 * rb, 8), 8), sl] = val

    def build_own(c, par, i, blk):
        build(par, 2 * c + i, blk, own_tiles(4 * c + 2 * i + par, blk))

    def build_edge(c, par, i, e):
        build(par, 2 * c + i, 6 * e, edge_tiles(c, 4 * c + 2 * i + par, e))

    def inside(c):
        lax.fori_loop(1, 6, lambda blk, x: (build_own(c, 0, 0, blk), x)[1], 0)

        def pair(i, x):
            for par in range(2):
                nxt = 1 if par else i

                def step(rb, y):
                    build_own(c, 1 - par, nxt, rb)
                    build_own(c, 1 - par, nxt, rb + 2)
                    interp(c, par, i, rb)
                    return y

                lax.fori_loop(1, 4, step, 0)
            return x

        lax.fori_loop(0, 2, pair, 0)

    def edges(c):
        lax.fori_loop(0, 2, lambda e, x: (build_edge(c, 0, 0, e), x)[1], 0)

        def pair(i, x):
            for par in range(2):
                nxt = 1 if par else i

                def step(e, y):
                    build_edge(c, 1 - par, nxt, e)
                    interp(c, par, i, 4 * e)
                    return y

                lax.fori_loop(0, 2, step, 0)
            return x

        lax.fori_loop(0, 2, pair, 0)

    def unpack_corners(slot):
        to_right, to_left = ccorn[2 * slot], ccorn[2 * slot + 1]
        for i in range(9):
            sl = pl.ds(8 + 8 * i + 8 * (i // 3), 8)
            halo[slot, 6, sl, :] = pltpu.roll(to_right, (-12 * i) % 128, 1)
            halo[slot, 0, sl, :] = pltpu.roll(to_left, (123 - 12 * i) % 128, 1)

    not_first = lambda act: pl.when(jnp.logical_not(first))(act)

    def swap(c, d, e, dev):
        other = lax.rem(lon + d, n_lon)
        h = hemi if e == 0 else 1 - hemi
        src = coeff.at[c, pl.ds(pl.multiple_of(other * 32, 32), 32), pl.ds(pl.multiple_of(h * 128, 128), 128)]
        return remote(src, got.at[c, 2 * d + e], xs_sem.at[c, 2 * d + e], xr_sem.at[c, 2 * d + e], dev)

    swaps = lambda c: [swap(c, d, e, dev) for (d, e), dev in zip(group, swap_to)]

    def inner_part(c):
        for cp in cols(c):
            cp.wait_recv()
        for i in range(4):
            for h in range(2):
                load(i, c, h).wait()
        inside(c)

        @pl.when(c < chunks - 1)
        def _():
            for kind in range(3):
                each(kind, lambda: (rows(kind, c).wait_send(), rows(kind, c + 1).start()) and None)

    def outer_part(c):
        not_first(lambda: rows(0, c).wait_recv())
        rows(1, c).wait_recv()

        @pl.when(c == 0)
        def _():
            for s in range(2):
                not_first(lambda: corner(0, s).wait_recv())
                corner(1, s).wait_recv()
            not_first(lambda: unpack_corners(0))
            unpack_corners(1)

        edges(c)
        gh, gl = split(grid[c])
        coeff[c] = three_pass(tab_h[...], tab_l[...], gh, gl, (((1,), (1,)), ((), ())))
        for s in swaps(c):
            s.start()

    def y_copy(c, d):
        return remote(part.at[c, pl.ds(4 * d, 4)], y_in.at[c, d - 1], ys_sem.at[c, d - 1], yr_sem.at[c, d - 1], y_to[d - 1])

    def z_copy(c, d):
        return remote(usum.at[c, d], z_in.at[c, d - 1], zs_sem.at[c, d - 1], zr_sem.at[c, d - 1], z_to[d - 1])

    others = range(1, side)
    y_send = lambda c: [y_copy(c, d) for d in others]
    z_send = lambda c: [z_copy(c, d) for d in others]
    sub_w = lax.broadcasted_iota(jnp.int32, (8, 640), 0)
    lane_w = lax.broadcasted_iota(jnp.int32, (8, 640), 1)

    def legendre_part(c):
        for s in swaps(c):
            s.wait_recv()
        same = coeff[c, pl.ds(pl.multiple_of(lon * 32, 32), 32), pl.ds(pl.multiple_of(hemi * 128, 128), 128)]
        other = got[c, 1]
        for d in range(1, n_lon):
            same = same + got[c, 2 * d]
            other = other + got[c, 2 * d + 1]
        sign = (1 - 2 * hemi).astype(F32)
        for e, z in enumerate((same + other, sign * (same - other))):
            for lv in range(2):
                moved_z = pltpu.roll(z, 88, 1) if lv else z
                for q in range(2):
                    for dup in range(2):
                        zs[pl.ds(8 * e + 4 * dup + 2 * q + lv, 16, stride=16), :] = moved_z[16 * q : 16 * q + 16]

        dims = (((1,), (0,)), ((), ()))

        def one(k, x):
            slot = lax.rem(yy + lax.div(k, side), side) * side + lax.rem(zz + lax.rem(k, side), side)
            m = wave[lon * 16 + slot]
            l_h, l_l = split(zs[pl.ds(pl.multiple_of(slot * 16, 16), 16), :][:, :40])
            even = ((lane_w + m) & 1) == 0
            res = []
            for hn in range(2):
                sl = pl.ds(640 * hn, 640)
                v = three_pass(l_h, l_l, leg_h[slot, :, sl], leg_l[slot, :, sl], dims)
                res.append(jnp.where(even, v[:8], v[8:]))
            part[c, k] = jnp.where(sub_w < 4, res[0], res[1])
            return x

        for d in (2, 1, 3, 0):
            lax.fori_loop(4 * d, 4 * d + 4, one, 0)
            if d:
                y_copy(c, d).start()

    def y_part(c):
        for s in y_send(c):
            s.wait_recv()
        for d in (2, 1, 3, 0):
            usum[c, d] = (part[c, d] + y_in[c, 0, d]) + (y_in[c, 1, d] + y_in[c, 2, d])
            if d:
                z_copy(c, d).start()

    def z_part(c):
        for s in z_send(c):
            s.wait_recv()
        total = (usum[c, 0] + z_in[c, 0]) + (z_in[c, 1] + z_in[c, 2])
        m = wave[lon * 16 + lat]
        degree = lane_w + jnp.where(sub_w < 4, 0, 640)
        h = jnp.where((sub_w & 1) == 0, helm[2 * c], helm[2 * c + 1])
        d = degree.astype(F32)
        total = jnp.where(degree >= m, total, 0.0) / (1.0 + h * (d * (d + 1.0)))
        for hn in range(2):
            for q in range(2):
                out[pl.ds(2 * c, 2), pl.ds(1280 * q + 640 * hn, 640)] = total[4 * hn + 2 * q : 4 * hn + 2 * q + 2]

    lax.fori_loop(0, chunks, lambda c, x: (inner_part(c), x)[1], 0)
    leg_fetch.wait()

    def split_leg(s, x):
        hi, lo = split(leg_v[s])
        leg_h[s], leg_l[s] = hi, lo
        return x

    lax.fori_loop(0, 16, split_leg, 0)


    def flow(c, x):
        outer_part(c)

        @pl.when(c > 0)
        def _():
            legendre_part(c - 1)

        return x

    lax.fori_loop(0, chunks, flow, 0)
    y_part(0)
    legendre_part(chunks - 1)
    y_part(1)
    y_part(2)
    z_part(0)
    z_part(1)
    z_part(2)

    for c in range(chunks):
        for cp in cols(c):
            cp.wait_send()
        if c == chunks - 1:
            for kind in range(3):
                each(kind, lambda: rows(kind, c).wait_send())
        for s in swaps(c) + y_send(c) + z_send(c):
            s.wait_send()
    for kind in range(3):
        each(kind, lambda: [corner(kind, s).wait_send() for s in range(2)] and None)


def whole(wave, helm, field, rsh, csh, rfr, cfr, leg, n_lat, n_lon):
    levels, rows, cols = field.shape
    V, S = pltpu.VMEM, pltpu.SMEM
    any_spec = pl.BlockSpec(memory_space=pl.ANY)
    sm = pl.BlockSpec(memory_space=S)
    B16, I32 = jnp.bfloat16, jnp.int32
    dma = pltpu.SemaphoreType.DMA
    c = 3
    edge = (5, 6 * levels, 128)
    blk = (8, 640)
    return pl.pallas_call(
        functools.partial(whole_kernel, n_lat, n_lon, math.isqrt(n_lat)),
        out_shape=jax.ShapeDtypeStruct((6, 2560), F32),
        in_specs=[sm, sm] + [any_spec] * 6,
        out_specs=pl.BlockSpec(memory_space=V),
        scratch_shapes=[
            V((levels, rows, cols + 256), F32), V(rsh.shape, I32), V(csh.shape, I32), V(rfr.shape, B16), V(cfr.shape, B16),
            V(edge, F32), V(edge, F32), V(edge, F32), V((6, 8, 128), F32),
            V((2, 7, 8 * levels + 16, 128), F32), V((4, 8, 128), F32),
            V((6, 60, rows + 16, 128), F32), V((6, 60, rows + 16, 128), F32),
            V((c, 256, cols), F32), V((128, cols), B16), V((128, cols), B16),
            V(leg.shape, F32), V(leg.shape, B16), V(leg.shape, B16),
            V((c, 128, 256), F32), V((c, 8, 32, 128), F32), V((256, 128), F32),
            V((c, 16) + blk, F32), V((c, 3, 4) + blk, F32), V((c, 4) + blk, F32), V((c, 3) + blk, F32),
            dma((c, 2)), dma((4, c, 2)), dma(()), dma((2, c)), dma((2, c)), dma((c,)), dma((c,)), dma((2, c)), dma((c,)), dma((6,)), dma((4,)),
            dma((c, 8)), dma((c, 8)), dma((c, 3)), dma((c, 3)), dma((c, 3)), dma((c, 3)),
        ],
        compiler_params=pltpu.CompilerParams(collective_id=0, has_side_effects=True, vmem_limit_bytes=60000 * 1024),
        name="whole",
    )(wave, helm, field, rsh, csh, rfr, cfr, leg)


def local(field, row_shift, col_shift, row_frac, col_frac, wave_map, legendre, helm_coef):
    n_lat, n_lon = lax.axis_size("lat"), lax.axis_size("lon")
    result = whole(wave_map, helm_coef, field[0], row_shift[0], col_shift[0], row_frac[0], col_frac[0], legendre, n_lat, n_lon)
    return result[:, None, None, :]


def solution(mesh):
    in_specs = (
        P("fold", None, "lat", "lon"),
        P("fold", None, "lat", "lon"),
        P("fold", None, "lat", "lon"),
        P("fold", None, "lat", "lon"),
        P("fold", None, "lat", "lon"),
        P(),
        P("lon", "lat", None),
        P("fold"),
    )
    return jax.shard_map(local, mesh=mesh, in_specs=in_specs, out_specs=P("fold", "lon", "lat", None), check_vma=False)
```

```python
import functools
import math

import jax
import jax.numpy as jnp
from jax import lax
from jax.experimental import pallas as pl
from jax.experimental.pallas import tpu as pltpu
from jax.sharding import PartitionSpec as P

MESH = pl.DeviceIdType.MESH
F32 = jnp.float32
SHIFTS = [c for c in range(-5, 7) if c != 0]


def lanes():
    return lax.broadcasted_iota(jnp.int32, (8, 128), 1)


def sublanes():
    return lax.broadcasted_iota(jnp.int32, (8, 128), 0)


def shifted_block(raw, store):
    lane = lanes()
    for t in range(5):
        store(25 + t, raw[t + 1])
    for c in SHIFTS:
        use = range(1, 7) if c > 0 else range(0, 6)
        moved = {t: pltpu.roll(raw[t], (-c) % 128, 1) for t in use}
        for t in range(1, 6):
            if c > 0:
                v = jnp.where(lane < 128 - c, moved[t], moved[t + 1])
            else:
                v = jnp.where(lane < -c, moved[t - 1], moved[t])
            store((c + 5) * 5 + t - 1, v)


def cubic(t):
    tm, tp, t2 = t - 1.0, t + 1.0, t - 2.0
    p, r = t * tm, tp * t2
    return (p * t2 * (-1.0 / 6.0), r * tm * 0.5, r * t * (-0.5), p * tp * (1.0 / 6.0))


def interp_tile(load, rb, rs, cs, u, v):
    idx = sublanes() + rs + 4
    low = idx < 8
    idx = idx & 7
    wr = cubic(u)
    s = cs + 4
    b0, b1, b2, b3 = (s & 1) != 0, (s & 2) != 0, (s & 4) != 0, s >= 8
    take = lambda x: jnp.take_along_axis(x, idx, axis=0, mode="promise_in_bounds")
    line, xs, ys = [], [], []
    for j in range(12):
        acc = None
        for a in range(4):
            g = jnp.where(low, take(load(j, rb * 8 + 3 + a)), take(load(j, rb * 8 + 11 + a))) * wr[a]
            acc = g if acc is None else acc + g
        line.append(acc)
        if 1 <= j <= 10:
            xs.append(jnp.where(b0, line[j], line[j - 1]))
            q = len(xs) - 1
            if q >= 2:
                ys.append(jnp.where(b1, xs[q], xs[q - 2]))
    wc = cubic(v)
    out = None
    for b in range(4):
        z = jnp.where(b2, ys[b + 4], ys[b])
        z = jnp.where(b3, line[b + 8], z)
        out = wc[b] * z if out is None else out + wc[b] * z
    return out


def three_pass(lh, ll, rh, rl, dims):
    dot = lambda a, b: lax.dot_general(a, b, dims, preferred_element_type=F32)
    n = lh.shape[0]
    both = dot(jnp.concatenate([lh, ll], axis=0), rh)
    return both[:n] + (dot(lh, rl) + both[n:])


def split(x):
    hi = x.astype(jnp.bfloat16)
    return hi, (x - hi.astype(F32)).astype(jnp.bfloat16)


def order_of_fetch(chunk):
    return (2 * chunk, 6 + 2 * chunk)


def whole_kernel(
    n_lat, n_lon, side,
    wave, helm, field, rsh, csh, rfr, cfr, leg, out,
    raw, rs_v, cs_v, rf_v, cf_v, tops, bots, mirs, cpack, halo, ccorn, moved_a, moved_b, grid, tab_h, tab_l,
    leg_v, leg_h, leg_l, coeff, got, zs, part, y_in, usum, z_in,
    loc_sem, in_sem, leg_sem, cs_sem, cr_sem, ts_sem, tr_sem, bs_sem, br_sem, ks_sem, kr_sem, xs_sem, xr_sem, ys_sem, yr_sem, zs_sem, zr_sem,
):
    lat, lon, fold = lax.axis_index("lat"), lax.axis_index("lon"), lax.axis_index("fold")
    up, down = lax.rem(lat + n_lat - 1, n_lat), lax.rem(lat + 1, n_lat)
    left, right = lax.rem(lon + n_lon - 1, n_lon), lax.rem(lon + 1, n_lon)
    hemi = lax.rem(fold, 2)
    mate = fold + 1 - 2 * hemi
    first, last = lat == 0, lat == n_lat - 1
    yy, zz = lax.div(lat, side), lax.rem(lat, side)
    y_at = [lax.rem(yy + d, side) for d in range(side)]
    z_at = [lax.rem(zz + d, side) for d in range(side)]
    chunks = 3

    def fetch(c, h):
        return pltpu.make_async_copy(
            field.at[pl.ds(order_of_fetch(c)[h], 2)], raw.at[pl.ds(4 * c + 2 * h, 2), :, pl.ds(128, 640)], loc_sem.at[c, h]
        )

    def load(i, c, h):
        src, dst = ((rsh, rs_v), (csh, cs_v), (rfr, rf_v), (cfr, cf_v))[i]
        return pltpu.make_async_copy(src.at[pl.ds(order_of_fetch(c)[h], 2)], dst.at[pl.ds(4 * c + 2 * h, 2)], in_sem.at[i, c, h])

    for c in range(chunks):
        for h in range(2):
            fetch(c, h).start()
    for c in range(chunks):
        for i in range(4):
            for h in range(2):
                load(i, c, h).start()
    leg_fetch = pltpu.make_async_copy(leg, leg_v, leg_sem)
    leg_fetch.start()
    barrier = pltpu.get_barrier_semaphore()
    peers = [{"lat": a, "lon": b} for a in (up, down) for b in (left, lon, right)]
    peers += [{"lon": b, "fold": mate} for b in (left, lon, right)]
    group = [(d, e) for d in range(n_lon) for e in range(2) if d or e]
    swap_to = [{"lon": lax.rem(lon + d, n_lon), "fold": mate if e else fold} for d, e in group]
    y_to = [{"lat": y_at[d] * side + zz} for d in range(1, side)]
    z_to = [{"lat": yy * side + z_at[d]} for d in range(1, side)]
    peers += swap_to + y_to + z_to
    for p in peers:
        pl.semaphore_signal(barrier, inc=1, device_id=p, device_id_type=MESH)

    def remote(src, dst, ssem, rsem, dev):
        return pltpu.make_async_remote_copy(src_ref=src, dst_ref=dst, send_sem=ssem, recv_sem=rsem, device_id=dev, device_id_type=MESH)

    def pack_rows(c):
        for l in range(4 * c, 4 * c + 4):
            for t in range(5):
                tile = pl.ds(128 + 128 * t, 128)
                tops[t, pl.ds(6 * l, 6), :] = raw[l, pl.ds(34, 6), tile]
                bots[t, pl.ds(6 * l, 6), :] = raw[l, pl.ds(0, 6), tile]

        @pl.when(last)
        def _():
            for l in range(4 * c, 4 * c + 4):
                for t in range(5):
                    for r in range(6):
                        mirs[t, pl.ds(6 * l + r, 1), :] = raw[l, pl.ds(39 - r, 1), pl.ds(128 + 128 * t, 128)]

    def pack_corner(k, rows):
        lane = lanes()
        a = b = jnp.zeros((8, 128), F32)
        for i in range(9):
            here = (lane >= 12 * i) & (lane < 12 * i + 12)
            a = jnp.where(here, pltpu.roll(rows[0, pl.ds(8 * i, 8), :], 12 * i, 1), a)
            b = jnp.where(here, pltpu.roll(rows[4, pl.ds(8 * i, 8), :], (12 * i + 5) % 128, 1), b)
        cpack[2 * k], cpack[2 * k + 1] = a, b

    def cols(c):
        lv = pl.ds(4 * c, 4)
        return (
            remote(raw.at[lv, :, pl.ds(128, 128)], raw.at[lv, :, pl.ds(768, 128)], cs_sem.at[0, c], cr_sem.at[0, c], {"lon": left}),
            remote(raw.at[lv, :, pl.ds(640, 128)], raw.at[lv, :, pl.ds(0, 128)], cs_sem.at[1, c], cr_sem.at[1, c], {"lon": right}),
        )

    def rows(kind, c):
        sl = pl.ds(pl.multiple_of(24 * c, 8), 24)
        if kind == 0:
            return remote(tops.at[:, sl, :], halo.at[0, pl.ds(1, 5), pl.ds(pl.multiple_of(8 + 32 * c, 8), 24), :], ts_sem.at[c], tr_sem.at[c], {"lat": down})
        src, dev = (bots, {"lat": up}) if kind == 1 else (mirs, {"fold": mate})
        return remote(src.at[:, sl, :], halo.at[1, pl.ds(1, 5), pl.ds(pl.multiple_of(8 + 32 * c, 8), 24), :], bs_sem.at[kind - 1, c], br_sem.at[c], dev)

    def corner(kind, side_):
        dev = {"lon": right if side_ else left}
        dev.update(({"lat": down}, {"lat": up}, {"fold": mate})[kind])
        slot = 0 if kind == 0 else 1
        return remote(cpack.at[2 * kind + side_], ccorn.at[2 * slot + side_], ks_sem.at[2 * kind + side_], kr_sem.at[2 * slot + side_], dev)

    def each(kind, act):
        cond = (jnp.logical_not(last), jnp.logical_not(first), last)[kind]

        @pl.when(cond)
        def _():
            act()

    sub, lane = sublanes(), lanes()
    for g in range(n_lon):
        for b in range(2):
            m = jnp.zeros((8, 128), jnp.int32)
            for k in range(8):
                m = jnp.where(sub == k, wave[16 * g + 8 * b + k], m)
            for t in range(5):
                turn = (m * (lane + (lon * 640 + 128 * t))).astype(F32)
                turn = turn - jnp.floor(turn * (1.0 / 2560.0)) * 2560.0
                angle = turn * (2.0 * math.pi / 2560.0)
                scale = 1.0 / math.sqrt(2560.0)
                for q, v in enumerate((jnp.cos(angle) * scale, jnp.sin(angle) * -scale)):
                    grid[0, pl.ds(32 * g + 16 * q + 8 * b, 8), pl.ds(128 * t, 128)] = v
    for c in range(chunks):
        for h in range(2):
            fetch(c, h).wait()
        pack_rows(c)
        if c == 0:
            pl.semaphore_wait(barrier, len(peers))
        if c == 0:
            for kind in range(3):
                each(kind, lambda: rows(kind, c).start())
        if c == 0:
            for cp in cols(c):
                cp.start()
    for kind, buf in enumerate((tops, bots)):
        pack_corner(kind, buf)
    each(2, lambda: pack_corner(2, mirs))
    for kind in range(3):
        each(kind, lambda: [corner(kind, s).start() for s in range(2)] and None)

    hi, lo = split(grid[0, pl.ds(0, 128), :])
    tab_h[...], tab_l[...] = hi, lo
    for c in range(chunks):
        for half in range(2):
            grid[c, pl.ds(128 * half + 80, 48), :] = jnp.zeros((48, 640), F32)
    @pl.when(first)
    def _():
        halo[0] = jnp.zeros_like(halo[0])

    moved = (moved_a, moved_b)

    def build(par, slot, blk, tiles):
        def store(i, v):
            moved[par][slot, i, pl.ds(pl.multiple_of(8 * blk, 8), 8), :] = v
        shifted_block(tiles, store)

    def own_tiles(l, blk):
        return [raw[l, pl.ds(pl.multiple_of(8 * (blk - 1), 8), 8), pl.ds(128 * t, 128)] for t in range(7)]

    def edge_tiles(c, l, e):
        return [halo[e, t, pl.ds(6 * l + 8 * c + 6 + 2 * e, 8), :] for t in range(7)]

    def interp(c, par, i, rb):
        l, slot = 4 * c + 2 * i + par, 2 * c + i
        for t in range(5):
            sl = pl.ds(128 * t, 128)
            args = [r[l, pl.ds(pl.multiple_of(8 * rb, 8), 8), sl] for r in (rs_v, cs_v, rf_v, cf_v)]
            val = interp_tile(
                lambda j, r0: moved[par][slot, j * 5 + t, pl.ds(r0, 8), :],
                rb, args[0], args[1], args[2].astype(F32), args[3].astype(F32),
            )
            grid[c, pl.ds(pl.multiple_of(128 * i + 40 * par + 8 * rb, 8), 8), sl] = val

    def build_own(c, par, i, blk):
        build(par, 2 * c + i, blk, own_tiles(4 * c + 2 * i + par, blk))

    def build_edge(c, par, i, e):
        build(par, 2 * c + i, 6 * e, edge_tiles(c, 4 * c + 2 * i + par, e))

    def inside(c):
        lax.fori_loop(1, 6, lambda blk, x: (build_own(c, 0, 0, blk), x)[1], 0)

        def pair(i, x):
            for par in range(2):
                nxt = 1 if par else i

                def step(rb, y):
                    build_own(c, 1 - par, nxt, rb)
                    build_own(c, 1 - par, nxt, rb + 2)
                    interp(c, par, i, rb)
                    return y

                lax.fori_loop(1, 4, step, 0)
            return x

        lax.fori_loop(0, 2, pair, 0)

    def edges(c):
        lax.fori_loop(0, 2, lambda e, x: (build_edge(c, 0, 0, e), x)[1], 0)

        def pair(i, x):
            for par in range(2):
                nxt = 1 if par else i

                def step(e, y):
                    build_edge(c, 1 - par, nxt, e)
                    interp(c, par, i, 4 * e)
                    return y

                lax.fori_loop(0, 2, step, 0)
            return x

        lax.fori_loop(0, 2, pair, 0)

    def unpack_corners(slot):
        to_right, to_left = ccorn[2 * slot], ccorn[2 * slot + 1]
        for i in range(9):
            sl = pl.ds(8 + 8 * i + 8 * (i // 3), 8)
            halo[slot, 6, sl, :] = pltpu.roll(to_right, (-12 * i) % 128, 1)
            halo[slot, 0, sl, :] = pltpu.roll(to_left, (123 - 12 * i) % 128, 1)

    not_first = lambda act: pl.when(jnp.logical_not(first))(act)

    def swap(c, d, e, dev):
        other = lax.rem(lon + d, n_lon)
        h = hemi if e == 0 else 1 - hemi
        src = coeff.at[c, pl.ds(pl.multiple_of(other * 32, 32), 32), pl.ds(pl.multiple_of(h * 128, 128), 128)]
        return remote(src, got.at[c, 2 * d + e], xs_sem.at[c, 2 * d + e], xr_sem.at[c, 2 * d + e], dev)

    swaps = lambda c: [swap(c, d, e, dev) for (d, e), dev in zip(group, swap_to)]

    def inner_part(c):
        for cp in cols(c):
            cp.wait_recv()

        @pl.when(c < chunks - 1)
        def _():
            for now, nxt in zip(cols(c), cols(c + 1)):
                now.wait_send()
                nxt.start()

        for i in range(4):
            for h in range(2):
                load(i, c, h).wait()
        inside(c)

        @pl.when(c < chunks - 1)
        def _():
            for kind in range(3):
                each(kind, lambda: (rows(kind, c).wait_send(), rows(kind, c + 1).start()) and None)

    def outer_part(c):
        not_first(lambda: rows(0, c).wait_recv())
        rows(1, c).wait_recv()

        @pl.when(c == 0)
        def _():
            for s in range(2):
                not_first(lambda: corner(0, s).wait_recv())
                corner(1, s).wait_recv()
            not_first(lambda: unpack_corners(0))
            unpack_corners(1)

        edges(c)
        gh, gl = split(grid[c])
        coeff[c] = three_pass(tab_h[...], tab_l[...], gh, gl, (((1,), (1,)), ((), ())))
        for s in swaps(c):
            s.start()

    def y_copy(c, d):
        return remote(part.at[c, pl.ds(4 * d, 4)], y_in.at[c, d - 1], ys_sem.at[c, d - 1], yr_sem.at[c, d - 1], y_to[d - 1])

    def z_copy(c, d):
        return remote(usum.at[c, d], z_in.at[c, d - 1], zs_sem.at[c, d - 1], zr_sem.at[c, d - 1], z_to[d - 1])

    others = range(1, side)
    y_send = lambda c: [y_copy(c, d) for d in others]
    z_send = lambda c: [z_copy(c, d) for d in others]
    sub_w = lax.broadcasted_iota(jnp.int32, (8, 640), 0)
    lane_w = lax.broadcasted_iota(jnp.int32, (8, 640), 1)

    def legendre_part(c):
        for s in swaps(c):
            s.wait_recv()
        same = coeff[c, pl.ds(pl.multiple_of(lon * 32, 32), 32), pl.ds(pl.multiple_of(hemi * 128, 128), 128)]
        other = got[c, 1]
        for d in range(1, n_lon):
            same = same + got[c, 2 * d]
            other = other + got[c, 2 * d + 1]
        sign = (1 - 2 * hemi).astype(F32)
        for e, z in enumerate((same + other, sign * (same - other))):
            for lv in range(2):
                moved_z = pltpu.roll(z, 88, 1) if lv else z
                for q in range(2):
                    for dup in range(2):
                        zs[pl.ds(8 * e + 4 * dup + 2 * q + lv, 16, stride=16), :] = moved_z[16 * q : 16 * q + 16]

        dims = (((1,), (0,)), ((), ()))

        def one(k, x):
            slot = lax.rem(yy + lax.div(k, side), side) * side + lax.rem(zz + lax.rem(k, side), side)
            m = wave[lon * 16 + slot]
            l_h, l_l = split(zs[pl.ds(pl.multiple_of(slot * 16, 16), 16), :][:, :40])
            even = ((lane_w + m) & 1) == 0
            res = []
            for hn in range(2):
                sl = pl.ds(640 * hn, 640)
                v = three_pass(l_h, l_l, leg_h[slot, :, sl], leg_l[slot, :, sl], dims)
                res.append(jnp.where(even, v[:8], v[8:]))
            part[c, k] = jnp.where(sub_w < 4, res[0], res[1])
            return x

        for d in (2, 1, 3, 0):
            lax.fori_loop(4 * d, 4 * d + 4, one, 0)
            if d:
                y_copy(c, d).start()

    def y_part(c):
        for s in y_send(c):
            s.wait_recv()
        for d in (2, 1, 3, 0):
            usum[c, d] = (part[c, d] + y_in[c, 0, d]) + (y_in[c, 1, d] + y_in[c, 2, d])
            if d:
                z_copy(c, d).start()

    def z_part(c):
        for s in z_send(c):
            s.wait_recv()
        total = (usum[c, 0] + z_in[c, 0]) + (z_in[c, 1] + z_in[c, 2])
        m = wave[lon * 16 + lat]
        degree = lane_w + jnp.where(sub_w < 4, 0, 640)
        h = jnp.where((sub_w & 1) == 0, helm[2 * c], helm[2 * c + 1])
        d = degree.astype(F32)
        total = jnp.where(degree >= m, total, 0.0) / (1.0 + h * (d * (d + 1.0)))
        for hn in range(2):
            for q in range(2):
                for lv in range(2):
                    r = 4 * hn + 2 * q + lv
                    for t in range(5):
                        out[pl.ds(20 * (2 * c + lv) + 10 * q + 5 * hn + t, 1), :] = total[r : r + 1, 128 * t : 128 * t + 128]

    def split_leg(s, x):
        hi, lo = split(leg_v[s])
        leg_h[s], leg_l[s] = hi, lo
        return x

    def flow(k, x):
        @pl.when(k < chunks)
        def _():
            inner_part(k)

        @pl.when(k == 1)
        def _():
            leg_fetch.wait()
            lax.fori_loop(0, 16, split_leg, 0)

        @pl.when(k > 0)
        def _():
            outer_part(k - 1)

        @pl.when(k > 1)
        def _():
            legendre_part(k - 2)

        return x

    lax.fori_loop(0, chunks + 1, flow, 0)
    y_part(0)
    legendre_part(chunks - 1)
    y_part(1)
    y_part(2)
    z_part(0)
    z_part(1)
    z_part(2)

    for c in range(chunks):
        if c == chunks - 1:
            for cp in cols(c):
                cp.wait_send()
        if c == chunks - 1:
            for kind in range(3):
                each(kind, lambda: rows(kind, c).wait_send())
        for s in swaps(c) + y_send(c) + z_send(c):
            s.wait_send()
    for kind in range(3):
        each(kind, lambda: [corner(kind, s).wait_send() for s in range(2)] and None)


def whole(wave, helm, field, rsh, csh, rfr, cfr, leg, n_lat, n_lon):
    levels, rows, cols = field.shape
    V, S = pltpu.VMEM, pltpu.SMEM
    any_spec = pl.BlockSpec(memory_space=pl.ANY)
    sm = pl.BlockSpec(memory_space=S)
    B16, I32 = jnp.bfloat16, jnp.int32
    dma = pltpu.SemaphoreType.DMA
    c = 3
    edge = (5, 6 * levels, 128)
    blk = (8, 640)
    return pl.pallas_call(
        functools.partial(whole_kernel, n_lat, n_lon, math.isqrt(n_lat)),
        out_shape=jax.ShapeDtypeStruct((120, 128), F32),
        in_specs=[sm, sm] + [any_spec] * 6,
        out_specs=pl.BlockSpec(memory_space=V),
        scratch_shapes=[
            V((levels, rows, cols + 256), F32), V(rsh.shape, I32), V(csh.shape, I32), V(rfr.shape, B16), V(cfr.shape, B16),
            V(edge, F32), V(edge, F32), V(edge, F32), V((6, 8, 128), F32),
            V((2, 7, 8 * levels + 16, 128), F32), V((4, 8, 128), F32),
            V((6, 60, rows + 16, 128), F32), V((6, 60, rows + 16, 128), F32),
            V((c, 256, cols), F32), V((128, cols), B16), V((128, cols), B16),
            V(leg.shape, F32), V(leg.shape, B16), V(leg.shape, B16),
            V((c, 128, 256), F32), V((c, 8, 32, 128), F32), V((256, 128), F32),
            V((c, 16) + blk, F32), V((c, 3, 4) + blk, F32), V((c, 4) + blk, F32), V((c, 3) + blk, F32),
            dma((c, 2)), dma((4, c, 2)), dma(()), dma((2, c)), dma((2, c)), dma((c,)), dma((c,)), dma((2, c)), dma((c,)), dma((6,)), dma((4,)),
            dma((c, 8)), dma((c, 8)), dma((c, 3)), dma((c, 3)), dma((c, 3)), dma((c, 3)),
        ],
        compiler_params=pltpu.CompilerParams(collective_id=0, has_side_effects=True, vmem_limit_bytes=60000 * 1024),
        name="whole",
    )(wave, helm, field, rsh, csh, rfr, cfr, leg)


def local(field, row_shift, col_shift, row_frac, col_frac, wave_map, legendre, helm_coef):
    n_lat, n_lon = lax.axis_size("lat"), lax.axis_size("lon")
    result = whole(wave_map, helm_coef, field[0], row_shift[0], col_shift[0], row_frac[0], col_frac[0], legendre, n_lat, n_lon)
    return result.reshape(helm_coef.shape[0], 1, 1, -1)


def solution(mesh):
    in_specs = (
        P("fold", None, "lat", "lon"),
        P("fold", None, "lat", "lon"),
        P("fold", None, "lat", "lon"),
        P("fold", None, "lat", "lon"),
        P("fold", None, "lat", "lon"),
        P(),
        P("lon", "lat", None),
        P("fold"),
    )
    return jax.shard_map(local, mesh=mesh, in_specs=in_specs, out_specs=P("fold", "lon", "lat", None), check_vma=False)
```
